8 devices in a mesh: replica: 1 (over z), model: 8 (over y, x, core).
Axes of the slice: x: 2, y: 2, z: 1, core: 2. Of those that a mesh axis runs over, the one named last changes fastest.
Arguments:
- x: bfloat16 [256, 4096], P('replica')
- w_query: bfloat16 [4096, 4096], P(None, 'model')
- w_key: bfloat16 [4096, 1024], replicated
- w_value: bfloat16 [4096, 1024], replicated
- w_out: bfloat16 [4096, 4096], P('model')
- k_cache: bfloat16 [256, 8, 1024, 128], P('replica')
- v_cache: bfloat16 [256, 8, 1024, 128], P('replica')
- lengths: int32 [256], P('replica')
Outputs:
- output 1: bfloat16 [256, 4096], P('replica')
- output 2: bfloat16 [256, 8, 128], P('replica')
- output 3: bfloat16 [256, 8, 128], P('replica')
All inputs are finite; a program needn't handle non-finite values.
Results may differ from the reference program's by a relative error of at most 0.00329967.
Values are sent between devices in bfloat16 or wider.
A program may use at most 4.25 GiB of HBM per device.

```python
import jax
import jax.numpy as jnp
from jax import lax

D_MODEL = 4096
NUM_HEADS = 32
KV_HEADS = 8
HEAD_DIM = 128
BATCH_SIZE = 256
CONTEXT_LEN = 1024


def draw_lengths(rng_key):
    key_perm, key_long, key_short = jax.random.split(rng_key, 3)
    perm_rank = jax.random.permutation(key_perm, BATCH_SIZE)
    long_count = max(1, BATCH_SIZE // 16)
    long_len = jax.random.randint(key_long, (BATCH_SIZE,), CONTEXT_LEN // 2, CONTEXT_LEN)
    short_len = jax.random.randint(key_short, (BATCH_SIZE,), 1, 33)
    seq_lens = jnp.where(perm_rank < 2 + long_count, long_len, short_len)
    seq_lens = jnp.where(perm_rank == 1, 1, seq_lens)
    seq_lens = jnp.where(perm_rank == 0, CONTEXT_LEN - 1, seq_lens)
    return seq_lens.astype(jnp.int32)


def setup_inputs(seed: int = 0, part: int = 0) -> dict:
    base_key = jax.random.key(seed)
    key_wq, key_wk, key_wv, key_wo = jax.random.split(base_key, 4)
    part_key = jax.random.fold_in(jax.random.key(seed + 1), part)
    key_x, key_kc, key_vc, key_mean, key_len = jax.random.split(part_key, 5)
    q_width = NUM_HEADS * HEAD_DIM
    kv_width = KV_HEADS * HEAD_DIM
    cache_shape = (BATCH_SIZE, KV_HEADS, CONTEXT_LEN, HEAD_DIM)
    x = jax.random.normal(key_x, (BATCH_SIZE, D_MODEL), jnp.float32).astype(jnp.bfloat16)
    w_query = (jax.random.normal(key_wq, (D_MODEL, q_width), jnp.float32) * D_MODEL ** -0.5).astype(jnp.bfloat16)
    w_key = (jax.random.normal(key_wk, (D_MODEL, kv_width), jnp.float32) * D_MODEL ** -0.5).astype(jnp.bfloat16)
    w_value = (jax.random.normal(key_wv, (D_MODEL, kv_width), jnp.float32) * D_MODEL ** -0.5).astype(jnp.bfloat16)
    w_out = (jax.random.normal(key_wo, (q_width, D_MODEL), jnp.float32) * q_width ** -0.5).astype(jnp.bfloat16)
    k_cache = (1.25 * jax.random.normal(key_kc, cache_shape, jnp.float32)).astype(jnp.bfloat16)
    v_mean = jax.random.normal(key_mean, (BATCH_SIZE, KV_HEADS, 1, HEAD_DIM), jnp.float32)
    v_cache = (jax.random.normal(key_vc, cache_shape, jnp.float32) + v_mean).astype(jnp.bfloat16)
    lengths = draw_lengths(key_len)
    return {"x": x, "w_query": w_query, "w_key": w_key, "w_value": w_value, "w_out": w_out, "k_cache": k_cache, "v_cache": v_cache, "lengths": lengths}


def reference(x, w_query, w_key, w_value, w_out, k_cache, v_cache, lengths):
    group_size = NUM_HEADS // KV_HEADS
    inv_sqrt = HEAD_DIM ** -0.5
    q_all = jnp.dot(x, w_query, preferred_element_type=jnp.float32).astype(jnp.bfloat16)
    k_new = jnp.dot(x, w_key, preferred_element_type=jnp.float32).astype(jnp.bfloat16).reshape(BATCH_SIZE, KV_HEADS, HEAD_DIM)
    v_new = jnp.dot(x, w_value, preferred_element_type=jnp.float32).astype(jnp.bfloat16).reshape(BATCH_SIZE, KV_HEADS, HEAD_DIM)
    q_heads = q_all.reshape(BATCH_SIZE, KV_HEADS, group_size, HEAD_DIM)
    positions = jnp.arange(CONTEXT_LEN)

    def one_sequence(item):
        q_seq, k_rows, v_rows, k_one, v_one, seq_len = item
        q_f32 = q_seq.astype(jnp.float32)
        scores = jnp.einsum("grd,gtd->grt", q_f32, k_rows.astype(jnp.float32)) * inv_sqrt
        score_new = jnp.einsum("grd,gd->gr", q_f32, k_one.astype(jnp.float32)) * inv_sqrt
        in_range = positions[None, None, :] < seq_len
        scores = jnp.where(in_range, scores, -jnp.inf)
        row_max = jnp.maximum(jnp.max(scores, axis=-1), score_new)
        weights = jnp.exp(scores - row_max[:, :, None])
        weight_new = jnp.exp(score_new - row_max)
        norm_sum = jnp.sum(weights, axis=-1) + weight_new
        out_sum = jnp.einsum("grt,gtd->grd", weights.astype(jnp.bfloat16).astype(jnp.float32), v_rows.astype(jnp.float32))
        out_sum = out_sum + weight_new.astype(jnp.bfloat16).astype(jnp.float32)[:, :, None] * v_one.astype(jnp.float32)[:, None, :]
        return (out_sum / norm_sum[:, :, None]).astype(jnp.bfloat16)

    attn_out = lax.map(one_sequence, (q_heads, k_cache, v_cache, k_new, v_new, lengths))
    o_flat = attn_out.reshape(BATCH_SIZE, NUM_HEADS * HEAD_DIM)
    y = (x.astype(jnp.float32) + jnp.dot(o_flat, w_out, preferred_element_type=jnp.float32)).astype(jnp.bfloat16)
    return (y, k_new, v_new)
```

```python
import functools

import jax
import jax.numpy as jnp
from jax import lax
from jax.experimental import pallas as pl
from jax.experimental.pallas import tpu as pltpu
from jax.sharding import PartitionSpec as P

BF16 = jnp.bfloat16
F32 = jnp.float32
SHORT = 32
PER_GROUP = 4
RING = 3
BLOCK = 256
K_CHUNKS = 4
CHUNK = 32
NT = (((1,), (1,)), ((), ()))


def project_and_attend_long(
    lens, x, wq, wk, wv, kc, vc,
    q_out, k1_out, v1_out, ol_out, lv_out,
    xbuf, wqbuf, wkbuf, wvbuf, kbuf, vbuf, idx, wsem, ksem, vsem,
):
    me = lax.axis_index("model")
    batch = lv_out.shape[0]
    heads, _, hd = q_out.shape
    context = kc.shape[2]
    blocks = context // BLOCK
    scale = hd ** -0.5
    depth = xbuf.shape[2]

    def loads(i):
        rows = pl.ds(i * depth, depth)
        cols = pl.ds(pl.multiple_of(me * hd, hd), hd)
        return (
            pltpu.make_async_copy(x.at[:, rows], xbuf.at[i], wsem.at[i, 0]),
            pltpu.make_async_copy(wq.at[rows, :], wqbuf.at[i], wsem.at[i, 1]),
            pltpu.make_async_copy(wk.at[rows, cols], wkbuf.at[i], wsem.at[i, 2]),
            pltpu.make_async_copy(wv.at[rows, cols], wvbuf.at[i], wsem.at[i, 3]),
        )

    for i in range(K_CHUNKS):
        for copy in loads(i):
            copy.start()

    def scan(b, n):
        length = lens[b]
        idx[n] = b
        lv_out[pl.ds(b, 1), :] = jnp.full((1, hd), length, jnp.int32)
        return n + (length > SHORT).astype(jnp.int32)

    n_long = lax.fori_loop(0, batch, scan, jnp.int32(0), unroll=8)
    n_groups = (n_long + PER_GROUP - 1) // PER_GROUP
    vbuf[...] = jnp.zeros_like(vbuf)

    def sequence(g, j):
        return idx[jnp.maximum(jnp.minimum(g * PER_GROUP + j, n_long - 1), 0)]

    def each_block(g, act):
        slot = lax.rem(g, RING)
        for j in range(PER_GROUP):
            b = sequence(g, j)
            length = lens[b]
            for t in range(blocks):
                rows = pl.ds(t * BLOCK, BLOCK)

                @pl.when(length > t * BLOCK)
                def _():
                    act(pltpu.make_async_copy(kc.at[b, me, rows, :], kbuf.at[slot, j, rows, :], ksem.at[slot, j, t]))
                    act(pltpu.make_async_copy(vc.at[b, me, rows, :], vbuf.at[slot, j, rows, :], vsem.at[slot, j, t]))

    for g in range(RING):
        @pl.when(g < n_groups)
        def _():
            each_block(jnp.int32(g), lambda copy: copy.start())

    q_acc = k_acc = v_acc = None
    for i in range(K_CHUNKS):
        for copy in loads(i):
            copy.wait()
        xs = xbuf[i]
        q_part = jnp.dot(xs, wqbuf[i], preferred_element_type=F32)
        k_part = jnp.dot(xs, wkbuf[i], preferred_element_type=F32)
        v_part = jnp.dot(xs, wvbuf[i], preferred_element_type=F32)
        for h in range(heads):
            piece = q_part[:, h * hd:(h + 1) * hd]
            q_out[h] = piece if i == 0 else q_out[h] + piece
        k1_out[...] = k_part if i == 0 else k1_out[...] + k_part
        v1_out[...] = v_part if i == 0 else v1_out[...] + v_part
    q_out[...] = q_out[...].astype(BF16).astype(F32)
    k1_out[...] = k1_out[...].astype(BF16).astype(F32)
    v1_out[...] = v1_out[...].astype(BF16).astype(F32)

    def attend(g, carry):
        slot = lax.rem(g, RING)
        each_block(g, lambda copy: copy.wait())
        results = []
        for j in range(PER_GROUP):
            b = sequence(g, j)
            length = lens[b]
            row = pl.ds(b, 1)
            q = jnp.concatenate([q_out[h, row, :] for h in range(heads)] * 2, axis=0)
            k1, v1 = k1_out[row, :], v1_out[row, :]
            s = lax.dot_general(q.astype(BF16), kbuf[slot, j], NT, preferred_element_type=F32) * scale
            s_new = jnp.sum(q * k1, axis=-1, keepdims=True) * scale
            s = jnp.where(lax.broadcasted_iota(jnp.int32, s.shape, 1) < length, s, -jnp.inf)
            m = jnp.maximum(jnp.max(s, axis=-1, keepdims=True), s_new)
            e = jnp.exp(s - m)
            e_new = jnp.exp(s_new - m)
            total = jnp.sum(e, axis=-1, keepdims=True) + e_new
            o = jnp.dot(e.astype(BF16), vbuf[slot, j], preferred_element_type=F32)
            o = (o + e_new.astype(BF16).astype(F32) * v1) / total
            results.append((row, o))
        for row, o in results:
            for h in range(heads):
                ol_out[h, row, :] = o[h:h + 1, :]

        @pl.when(g + RING < n_groups)
        def _():
            each_block(g + RING, lambda copy: copy.start())

        return carry

    lax.fori_loop(0, n_groups, attend, 0)


def attend_short_and_reduce(
    q_ref, k1_ref, v1_ref, ol_ref, lv_ref, x, wo, wk, wv, kc, vc,
    y_out, kn_out, vn_out,
    xbuf, wobuf, wkv, kbuf, vbuf, obuf, part, got_core, got_one, got_two, ybuf, kvbuf,
    load_sem, send_sem, recv_sem, store_sem,
):
    me = lax.axis_index("model")
    core = me % 2
    px = (me // 2) % 2
    py = me // 4
    flip_x = me + 2 - 4 * px
    flip_y = me + 4 - 8 * py
    other_core = 1 - core
    partner = me + 1 - 2 * core
    near_one = other_core * flip_x + core * flip_y
    near_two = other_core * flip_y + core * flip_x
    a = other_core * px + core * py
    b = other_core * py + core * px
    base = 4 * core
    mine = base + 2 * a + b
    heads, batch, hd = q_ref.shape
    width = part.shape[3]
    chunks = batch // CHUNK
    kv_width = wkv.shape[1] // 2
    kv_cols = 2 * kv_width // 8
    scale = hd ** -0.5

    loads = (
        pltpu.make_async_copy(kc.at[:, me, pl.ds(0, SHORT), :], kbuf, load_sem.at[0]),
        pltpu.make_async_copy(vc.at[:, me, pl.ds(0, SHORT), :], vbuf, load_sem.at[1]),
        pltpu.make_async_copy(wo, wobuf, load_sem.at[2]),
        pltpu.make_async_copy(x, xbuf, load_sem.at[3]),
        pltpu.make_async_copy(wk, wkv.at[:, pl.ds(0, kv_width)], load_sem.at[4]),
        pltpu.make_async_copy(wv, wkv.at[:, pl.ds(kv_width, kv_width)], load_sem.at[5]),
    )
    for copy in loads:
        copy.start()

    barrier = pltpu.get_barrier_semaphore()
    for other in (partner, near_one, near_two):
        pl.semaphore_signal(barrier, inc=1, device_id={"model": other}, device_id_type=pl.DeviceIdType.MESH)
    pl.semaphore_wait(barrier, 3)

    def send(stage, r, src, dst, other):
        return pltpu.make_async_remote_copy(
            src_ref=src, dst_ref=dst, send_sem=send_sem.at[stage, r], recv_sem=recv_sem.at[stage, r],
            device_id={"model": other}, device_id_type=pl.DeviceIdType.MESH,
        )

    def rows_of(r):
        return pl.ds(pl.multiple_of(r * CHUNK, CHUNK), CHUNK)

    def cols_of(f, count):
        return pl.ds(pl.multiple_of(f * width, width), count * width)

    def to_core(r):
        return send(0, r, part.at[r, pl.ds(4 * other_core, 4)], got_core.at[r], partner)

    def to_one(r):
        return send(1, r, part.at[r, pl.ds(base + 2 * (1 - a), 2)], got_one.at[r], near_one)

    def to_two(r):
        return send(2, r, part.at[r, base + 2 * a + 1 - b], got_two.at[r], near_two)

    def y_to_two(r):
        view = ybuf.at[rows_of(r), cols_of(mine, 1)]
        return send(3, r, view, view, near_two)

    def y_to_one(r):
        view = ybuf.at[rows_of(r), cols_of(base + 2 * a, 2)]
        return send(4, r, view, view, near_one)

    def y_to_core(r):
        view = ybuf.at[rows_of(r), cols_of(base, 4)]
        return send(5, r, view, view, partner)

    def y_store(r):
        return pltpu.make_async_copy(ybuf.at[rows_of(r), :], y_out.at[rows_of(r), :], store_sem.at[r])

    def attend(r):
        for g in range(CHUNK // 8):
            rows = pl.ds(pl.multiple_of(r * CHUNK + g * 8, 8), 8)
            q = jnp.concatenate([q_ref[h, rows, :] for h in range(heads)], axis=0)
            k1 = jnp.concatenate([k1_ref[rows, :]] * heads, axis=0)
            v1 = jnp.concatenate([v1_ref[rows, :]] * heads, axis=0)
            lens = jnp.concatenate([lv_ref[rows, :]] * heads, axis=0)
            k = kbuf[rows].reshape(8 * SHORT, hd)
            v = vbuf[rows].reshape(8 * SHORT, hd)
            s = lax.dot_general(q.astype(BF16), k, NT, preferred_element_type=F32) * scale
            s_new = jnp.sum(q * k1, axis=-1, keepdims=True) * scale
            lane = lax.broadcasted_iota(jnp.int32, s.shape, 1)
            line = lax.broadcasted_iota(jnp.int32, s.shape, 0)
            slot = lane - (line % 8) * SHORT
            wide = jnp.concatenate([lens] * (s.shape[1] // hd), axis=1)
            s = jnp.where((slot >= 0) & (slot < jnp.minimum(wide, SHORT)), s, -jnp.inf)
            m = jnp.maximum(jnp.max(s, axis=-1, keepdims=True), s_new)
            e = jnp.exp(s - m)
            e_new = jnp.exp(s_new - m)
            total = jnp.sum(e, axis=-1, keepdims=True) + e_new
            o = jnp.dot(e.astype(BF16), v, preferred_element_type=F32)
            o = (o + e_new.astype(BF16).astype(F32) * v1) / total
            for h in range(heads):
                picked = jnp.where(lens[:8] > SHORT, ol_ref[h, rows, :], o[h * 8:(h + 1) * 8])
                obuf[pl.ds(g * 8, 8), pl.ds(h * hd, hd)] = picked

        o_rows = obuf[...].astype(BF16)

        def piece(f, carry):
            part[r, f] = jnp.dot(o_rows, wobuf[:, cols_of(f, 1)], preferred_element_type=F32)
            return carry

        lax.fori_loop(0, 8, piece, 0)

    def new_rows(t):
        cols = pl.ds(pl.multiple_of(t * kv_cols, kv_cols), kv_cols)
        kvbuf[:, cols] = jnp.dot(xbuf[...], wkv[:, cols], preferred_element_type=F32).astype(BF16)

    for copy in loads[:4]:
        copy.wait()

    def step(t, carry):
        @pl.when((t >= 6) & (t < chunks + 6))
        def _():
            y_to_core(t - 6).wait()
            y_store(t - 6).start()

        @pl.when((t >= 5) & (t < chunks + 5))
        def _():
            y_to_one(t - 5).wait()
            y_to_core(t - 5).start()

        @pl.when((t >= 4) & (t < chunks + 4))
        def _():
            y_to_two(t - 4).wait()
            y_to_one(t - 4).start()

        @pl.when((t >= 3) & (t < chunks + 3))
        def _():
            r = t - 3
            to_two(r).wait()
            total = part[r, mine] + got_two[r]
            total = total + xbuf[rows_of(r), cols_of(mine, 1)].astype(F32)
            ybuf[rows_of(r), cols_of(mine, 1)] = total.astype(BF16)
            y_to_two(r).start()

        @pl.when((t >= 2) & (t < chunks + 2))
        def _():
            r = t - 2
            to_one(r).wait()
            part[r, pl.ds(base + 2 * a, 2)] += got_one[r]
            to_two(r).start()

        @pl.when((t >= 1) & (t < chunks + 1))
        def _():
            r = t - 1
            to_core(r).wait()
            part[r, pl.ds(base, 4)] += got_core[r]
            to_one(r).start()

        @pl.when(t < chunks)
        def _():
            attend(t)
            to_core(t).start()

        @pl.when(t == 3)
        def _():
            loads[4].wait()
            loads[5].wait()

        @pl.when((t >= 3) & (t < 11))
        def _():
            new_rows(t - 3)

        return carry

    lax.fori_loop(0, chunks + 6, step, 0)
    k_store = pltpu.make_async_copy(kvbuf.at[:, pl.ds(0, kv_width)], kn_out, load_sem.at[0])
    v_store = pltpu.make_async_copy(kvbuf.at[:, pl.ds(kv_width, kv_width)], vn_out, load_sem.at[1])
    k_store.start()
    v_store.start()
    for r in range(chunks):
        y_store(r).wait()
    k_store.wait()
    v_store.wait()


def solution(mesh):
    def local_step(x, w_query, w_key, w_value, w_out, k_cache, v_cache, lengths):
        batch, width = x.shape
        kv_heads, context, hd = k_cache.shape[1:]
        heads = w_query.shape[1] // hd
        kv_width = kv_heads * hd
        depth = width // K_CHUNKS
        piece = width // 8
        chunks = batch // CHUNK
        vmem = pl.BlockSpec(memory_space=pltpu.VMEM)
        hbm = pl.BlockSpec(memory_space=pl.ANY)
        sds = jax.ShapeDtypeStruct

        q, k1, v1, ol, lv = pl.pallas_call(
            project_and_attend_long,
            out_shape=(
                sds((heads, batch, hd), F32), sds((batch, hd), F32), sds((batch, hd), F32),
                sds((heads, batch, hd), F32), sds((batch, hd), jnp.int32),
            ),
            in_specs=[pl.BlockSpec(memory_space=pltpu.SMEM)] + [hbm] * 6,
            out_specs=[vmem] * 5,
            scratch_shapes=[
                pltpu.VMEM((K_CHUNKS, batch, depth), BF16),
                pltpu.VMEM((K_CHUNKS, depth, heads * hd), BF16),
                pltpu.VMEM((K_CHUNKS, depth, hd), BF16),
                pltpu.VMEM((K_CHUNKS, depth, hd), BF16),
                pltpu.VMEM((RING, PER_GROUP, context, hd), BF16),
                pltpu.VMEM((RING, PER_GROUP, context, hd), BF16),
                pltpu.SMEM((batch,), jnp.int32),
                pltpu.SemaphoreType.DMA((K_CHUNKS, 4)),
                pltpu.SemaphoreType.DMA((RING, PER_GROUP, context // BLOCK)),
                pltpu.SemaphoreType.DMA((RING, PER_GROUP, context // BLOCK)),
            ],
            compiler_params=pltpu.CompilerParams(vmem_limit_bytes=48 * 2**20),
            name="project_and_attend_long",
        )(lengths, x, w_query, w_key, w_value, k_cache, v_cache)

        y, kn, vn = pl.pallas_call(
            attend_short_and_reduce,
            out_shape=(sds((batch, width), BF16), sds((batch, kv_width), BF16), sds((batch, kv_width), BF16)),
            in_specs=[vmem] * 5 + [hbm] * 6,
            out_specs=[hbm] * 3,
            scratch_shapes=[
                pltpu.VMEM((batch, width), BF16),
                pltpu.VMEM((heads * hd, width), BF16),
                pltpu.VMEM((width, 2 * kv_width), BF16),
                pltpu.VMEM((batch, SHORT, hd), BF16),
                pltpu.VMEM((batch, SHORT, hd), BF16),
                pltpu.VMEM((CHUNK, heads * hd), F32),
                pltpu.VMEM((chunks, 8, CHUNK, piece), F32),
                pltpu.VMEM((chunks, 4, CHUNK, piece), F32),
                pltpu.VMEM((chunks, 2, CHUNK, piece), F32),
                pltpu.VMEM((chunks, CHUNK, piece), F32),
                pltpu.VMEM((batch, width), BF16),
                pltpu.VMEM((batch, 2 * kv_width), BF16),
                pltpu.SemaphoreType.DMA((6,)),
                pltpu.SemaphoreType.DMA((6, chunks)),
                pltpu.SemaphoreType.DMA((6, chunks)),
                pltpu.SemaphoreType.DMA((chunks,)),
            ],
            compiler_params=pltpu.CompilerParams(
                vmem_limit_bytes=60 * 2**20, collective_id=0, has_side_effects=True
            ),
            name="attend_short_and_reduce",
        )(q, k1, v1, ol, lv, x, w_out, w_key, w_value, k_cache, v_cache)
        return y, kn.reshape(batch, kv_heads, hd), vn.reshape(batch, kv_heads, hd)

    rows_spec = P("replica")
    return jax.shard_map(
        local_step,
        mesh=mesh,
        in_specs=(P("replica", None), P(None, "model"), P(), P(), P("model", None), rows_spec, rows_spec, rows_spec),
        out_specs=(rows_spec, rows_spec, rows_spec),
        check_vma=False,
    )
```

```python
import functools

import jax
import jax.numpy as jnp
from jax import lax
from jax.experimental import pallas as pl
from jax.experimental.pallas import tpu as pltpu
from jax.sharding import PartitionSpec as P

BF16 = jnp.bfloat16
F32 = jnp.float32
SHORT = 32
PER_GROUP = 4
RING = 3
BLOCK = 256
K_CHUNKS = 4
BLOCK_ROWS = 64
KV_STEPS = 8
PARTS = ((0, 64), (64, 192))
CHUNKS = tuple((32 * i, 32) for i in range(8))
ATTEND, PROJECT, NEW = 6, 7, 8
ORDER = (
    (ATTEND, 0), (PROJECT, 0), (ATTEND, 1), (0, 0), (0, 1), (PROJECT, 1),
    (0, 2), (1, 0), (0, 3), (0, 4), (NEW, 0), (0, 5), (1, 1), (0, 6), (0, 7), (NEW, 1), (2, 0), (NEW, 2),
    (1, 2), (2, 1), (NEW, 3), (1, 3), (3, 0), (NEW, 4), (1, 4), (2, 2), (3, 1), (2, 3), (NEW, 5), (1, 5), (2, 4),
    (3, 2), (3, 3), (NEW, 6), (1, 6), (2, 5), (3, 4), (NEW, 7), (1, 7), (2, 6), (4, 0), (3, 5), (4, 1), (5, 0),
    (2, 7), (5, 1), (4, 2), (3, 6), (4, 3), (5, 2), (4, 4), (5, 3), (3, 7), (4, 5), (5, 4), (4, 6), (5, 5),
    (5, 6), (4, 7), (5, 7),
)
NT = (((1,), (1,)), ((), ()))


def project_and_attend_long(
    lens_hbm, x, wq, wk, wv, wo, kc, vc,
    q_out, k1_out, v1_out, ol_out, lv_out, ks_out, vs_out, wo_out,
    xbuf, wqbuf, wkbuf, wvbuf, kbuf, vbuf, lens, idx, wsem, ksem, vsem, next_sem,
):
    me = lax.axis_index("model")
    batch = lv_out.shape[0]
    heads, _, hd = q_out.shape
    context = kc.shape[2]
    blocks = context // BLOCK
    scale = hd ** -0.5
    depth = xbuf.shape[2]

    def loads(i):
        rows = pl.ds(i * depth, depth)
        cols = pl.ds(pl.multiple_of(me * hd, hd), hd)
        return (
            pltpu.make_async_copy(x.at[:, rows], xbuf.at[i], wsem.at[i, 0]),
            pltpu.make_async_copy(wq.at[rows, :], wqbuf.at[i], wsem.at[i, 1]),
            pltpu.make_async_copy(wk.at[rows, cols], wkbuf.at[i], wsem.at[i, 2]),
            pltpu.make_async_copy(wv.at[rows, cols], wvbuf.at[i], wsem.at[i, 3]),
        )

    lens_load = pltpu.make_async_copy(lens_hbm, lens, wsem.at[0, 4])
    lens_load.start()
    for i in range(K_CHUNKS):
        for copy in loads(i):
            copy.start()
    lens_load.wait()

    def scan(b, n):
        length = lens[b]
        idx[n] = b
        lv_out[pl.ds(b, 1), :] = jnp.full((1, hd), length, jnp.int32)
        return n + (length > SHORT).astype(jnp.int32)

    n_long = lax.fori_loop(0, batch, scan, jnp.int32(0), unroll=8)
    n_groups = (n_long + PER_GROUP - 1) // PER_GROUP
    vbuf[...] = jnp.zeros_like(vbuf)

    def sequence(g, j):
        return idx[jnp.maximum(jnp.minimum(g * PER_GROUP + j, n_long - 1), 0)]

    def each_block(g, act):
        slot = lax.rem(g, RING)
        for j in range(PER_GROUP):
            b = sequence(g, j)
            length = lens[b]
            for t in range(blocks):
                rows = pl.ds(t * BLOCK, BLOCK)

                @pl.when(length > t * BLOCK)
                def _():
                    act(pltpu.make_async_copy(kc.at[b, me, rows, :], kbuf.at[slot, j, rows, :], ksem.at[slot, j, t]))
                    act(pltpu.make_async_copy(vc.at[b, me, rows, :], vbuf.at[slot, j, rows, :], vsem.at[slot, j, t]))

    for g in range(RING):
        @pl.when(g < n_groups)
        def _():
            each_block(jnp.int32(g), lambda copy: copy.start())

    ahead = (
        pltpu.make_async_copy(kc.at[:, me, pl.ds(0, SHORT), :], ks_out, next_sem.at[0]),
        pltpu.make_async_copy(vc.at[:, me, pl.ds(0, SHORT), :], vs_out, next_sem.at[1]),
        pltpu.make_async_copy(wo, wo_out, next_sem.at[2]),
    )
    for copy in ahead:
        copy.start()

    for i in range(K_CHUNKS):
        for copy in loads(i):
            copy.wait()
        xs = xbuf[i]
        q_part = jnp.dot(xs, wqbuf[i], preferred_element_type=F32)
        k_part = jnp.dot(xs, wkbuf[i], preferred_element_type=F32)
        v_part = jnp.dot(xs, wvbuf[i], preferred_element_type=F32)
        for h in range(heads):
            piece = q_part[:, h * hd:(h + 1) * hd]
            q_out[h] = piece if i == 0 else q_out[h] + piece
        k1_out[...] = k_part if i == 0 else k1_out[...] + k_part
        v1_out[...] = v_part if i == 0 else v1_out[...] + v_part
    q_out[...] = q_out[...].astype(BF16).astype(F32)
    k1_out[...] = k1_out[...].astype(BF16).astype(F32)
    v1_out[...] = v1_out[...].astype(BF16).astype(F32)

    def attend(g, carry):
        slot = lax.rem(g, RING)
        each_block(g, lambda copy: copy.wait())
        results = []
        for j in range(PER_GROUP):
            b = sequence(g, j)
            length = lens[b]
            row = pl.ds(b, 1)
            q = jnp.concatenate([q_out[h, row, :] for h in range(heads)] * 2, axis=0)
            k1, v1 = k1_out[row, :], v1_out[row, :]
            s = lax.dot_general(q.astype(BF16), kbuf[slot, j], NT, preferred_element_type=F32) * scale
            s_new = jnp.sum(q * k1, axis=-1, keepdims=True) * scale
            s = jnp.where(lax.broadcasted_iota(jnp.int32, s.shape, 1) < length, s, -jnp.inf)
            m = jnp.maximum(jnp.max(s, axis=-1, keepdims=True), s_new)
            e = jnp.exp(s - m)
            e_new = jnp.exp(s_new - m)
            total = jnp.sum(e, axis=-1, keepdims=True) + e_new
            o = jnp.dot(e.astype(BF16), vbuf[slot, j], preferred_element_type=F32)
            o = (o + e_new.astype(BF16).astype(F32) * v1) / total
            results.append((row, o))
        for row, o in results:
            for h in range(heads):
                ol_out[h, row, :] = o[h:h + 1, :]

        @pl.when(g + RING < n_groups)
        def _():
            each_block(g + RING, lambda copy: copy.start())

        return carry

    lax.fori_loop(0, n_groups, attend, 0)
    for copy in ahead:
        copy.wait()


def attend_short_and_reduce(
    q_ref, k1_ref, v1_ref, ol_ref, lv_ref, kbuf, vbuf, wobuf, x, wk, wv,
    y_out, kn_out, vn_out,
    xbuf, wkv, obuf, part, got_core, got_one, got_two, kvbuf,
    load_sem, send_sem, recv_sem,
):
    me = lax.axis_index("model")
    core = me % 2
    px = (me // 2) % 2
    py = me // 4
    flip_x = me + 2 - 4 * px
    flip_y = me + 4 - 8 * py
    other_core = 1 - core
    partner = me + 1 - 2 * core
    near_one = other_core * flip_x + core * flip_y
    near_two = other_core * flip_y + core * flip_x
    a = other_core * px + core * py
    b = other_core * py + core * px
    base = 4 * core
    mine = base + 2 * a + b
    heads, batch, hd = q_ref.shape
    width = part.shape[2]
    kv_width = wkv.shape[1] // 2
    kv_heads = kv_width // hd
    slice_heads = 2 * kv_heads // KV_STEPS
    scale = hd ** -0.5

    loads = (
        pltpu.make_async_copy(x, xbuf, load_sem.at[0]),
        pltpu.make_async_copy(wk, wkv.at[:, pl.ds(0, kv_width)], load_sem.at[1]),
        pltpu.make_async_copy(wv, wkv.at[:, pl.ds(kv_width, kv_width)], load_sem.at[2]),
    )
    for copy in loads:
        copy.start()

    barrier = pltpu.get_barrier_semaphore()
    for other in (partner, near_one, near_two):
        pl.semaphore_signal(barrier, inc=1, device_id={"model": other}, device_id_type=pl.DeviceIdType.MESH)

    def rows_of(r):
        first, count = CHUNKS[r]
        return pl.ds(first, count)

    def cols_of(f, count):
        return pl.ds(pl.multiple_of(f * width, width), count * width)

    def send(stage, r):
        rows = rows_of(r)
        if stage == 0:
            src, dst, other = part.at[pl.ds(4 * other_core, 4), rows], got_core.at[:, rows], partner
        elif stage == 1:
            src, dst, other = part.at[pl.ds(base + 2 * (1 - a), 2), rows], got_one.at[:, rows], near_one
        elif stage == 2:
            src, dst, other = part.at[base + 2 * a + 1 - b, rows], got_two.at[rows], near_two
        elif stage == 3:
            src = dst = y_out.at[rows, cols_of(mine, 1)]
            other = near_two
        elif stage == 4:
            src = dst = y_out.at[rows, cols_of(base + 2 * a, 2)]
            other = near_one
        else:
            src = dst = y_out.at[rows, cols_of(base, 4)]
            other = partner
        return pltpu.make_async_remote_copy(
            src_ref=src, dst_ref=dst, send_sem=send_sem.at[stage, r], recv_sem=recv_sem.at[stage, r],
            device_id={"model": other}, device_id_type=pl.DeviceIdType.MESH,
        )

    def advance(stage, r):
        rows = rows_of(r)
        send(stage, r).wait()
        if stage == 0:
            part[pl.ds(base, 4), rows] += got_core[:, rows]
        elif stage == 1:
            part[pl.ds(base + 2 * a, 2), rows] += got_one[:, rows]
        elif stage == 2:
            total = part[mine, rows] + got_two[rows]
            total = total + xbuf[rows, cols_of(mine, 1)].astype(F32)
            y_out[rows, cols_of(mine, 1)] = total.astype(BF16)
        if stage < 5:
            send(stage + 1, r).start()

    def attend_block(first):
        for g in range(BLOCK_ROWS // 8):
            rows = pl.ds(pl.multiple_of(first + g * 8, 8), 8)
            q = jnp.concatenate([q_ref[h, rows, :] for h in range(heads)], axis=0)
            k1 = jnp.concatenate([k1_ref[rows, :]] * heads, axis=0)
            v1 = jnp.concatenate([v1_ref[rows, :]] * heads, axis=0)
            lens = jnp.concatenate([lv_ref[rows, :]] * heads, axis=0)
            k = kbuf[rows].reshape(8 * SHORT, hd)
            v = vbuf[rows].reshape(8 * SHORT, hd)
            s = lax.dot_general(q.astype(BF16), k, NT, preferred_element_type=F32) * scale
            s_new = jnp.sum(q * k1, axis=-1, keepdims=True) * scale
            lane = lax.broadcasted_iota(jnp.int32, s.shape, 1)
            line = lax.broadcasted_iota(jnp.int32, s.shape, 0)
            slot = lane - (line % 8) * SHORT
            wide = jnp.concatenate([lens] * (s.shape[1] // hd), axis=1)
            s = jnp.where((slot >= 0) & (slot < jnp.minimum(wide, SHORT)), s, -jnp.inf)
            m = jnp.maximum(jnp.max(s, axis=-1, keepdims=True), s_new)
            e = jnp.exp(s - m)
            e_new = jnp.exp(s_new - m)
            total = jnp.sum(e, axis=-1, keepdims=True) + e_new
            o = jnp.dot(e.astype(BF16), v, preferred_element_type=F32)
            o = (o + e_new.astype(BF16).astype(F32) * v1) / total
            for h in range(heads):
                picked = jnp.where(lens[:8] > SHORT, ol_ref[h, rows, :], o[h * 8:(h + 1) * 8])
                obuf[rows, pl.ds(h * hd, hd)] = picked

    def attend(first, count):
        if count == BLOCK_ROWS:
            attend_block(first)
        else:
            def body(i, carry):
                attend_block(first + i * BLOCK_ROWS)
                return carry

            lax.fori_loop(0, count // BLOCK_ROWS, body, 0)

    def project_out(first, count):
        rows = pl.ds(first, count)
        o_rows = obuf[rows, :].astype(BF16)
        for f in range(8):
            part[f, rows] = jnp.dot(o_rows, wobuf[:, f * width:(f + 1) * width], preferred_element_type=F32)

    def new_rows(t):
        if t == 0:
            loads[0].wait()
            loads[1].wait()
            loads[2].wait()
        cols = pl.ds(t * slice_heads * hd, slice_heads * hd)
        fresh = jnp.dot(xbuf[...], wkv[:, cols], preferred_element_type=F32)
        for h in range(slice_heads):
            kvbuf[:, (t * slice_heads + h) % kv_heads, :] = fresh[:, h * hd:(h + 1) * hd]
        if t == KV_STEPS // 2 - 1:
            kn_out[...] = kvbuf[...].astype(BF16)
        if t == KV_STEPS - 1:
            vn_out[...] = kvbuf[...].astype(BF16)

    for op, i in ORDER:
        if op == ATTEND:
            attend(*PARTS[i])
        elif op == PROJECT:
            project_out(*PARTS[i])
            if i == 0:
                pl.semaphore_wait(barrier, 3)
            for r, (first, _) in enumerate(CHUNKS):
                if PARTS[i][0] <= first < PARTS[i][0] + PARTS[i][1]:
                    send(0, r).start()
        elif op == NEW:
            new_rows(i)
        else:
            advance(op, i)


def copy_out(y, kn, vn, y_out, kn_out, vn_out, sem):
    copies = [
        pltpu.make_async_copy(src, dst, sem.at[i])
        for i, (src, dst) in enumerate(((y, y_out), (kn, kn_out), (vn, vn_out)))
    ]
    for copy in copies:
        copy.start()
    for copy in copies:
        copy.wait()


def solution(mesh):
    def local_step(x, w_query, w_key, w_value, w_out, k_cache, v_cache, lengths):
        batch, width = x.shape
        kv_heads, context, hd = k_cache.shape[1:]
        heads = w_query.shape[1] // hd
        kv_width = kv_heads * hd
        depth = width // K_CHUNKS
        piece = width // 8
        vmem = pl.BlockSpec(memory_space=pltpu.VMEM)
        hbm = pl.BlockSpec(memory_space=pltpu.HBM)
        sds = jax.ShapeDtypeStruct
        x, w_query, w_key, w_value, w_out, k_cache, v_cache, lengths = (
            pltpu.with_memory_space_constraint(array, pltpu.HBM)
            for array in (x, w_query, w_key, w_value, w_out, k_cache, v_cache, lengths)
        )

        ahead = pl.pallas_call(
            project_and_attend_long,
            out_shape=(
                sds((heads, batch, hd), F32), sds((batch, hd), F32), sds((batch, hd), F32),
                sds((heads, batch, hd), F32), sds((batch, hd), jnp.int32),
                sds((batch, SHORT, hd), BF16), sds((batch, SHORT, hd), BF16), sds((heads * hd, width), BF16),
            ),
            in_specs=[hbm] * 8,
            out_specs=[vmem] * 8,
            scratch_shapes=[
                pltpu.VMEM((K_CHUNKS, batch, depth), BF16),
                pltpu.VMEM((K_CHUNKS, depth, heads * hd), BF16),
                pltpu.VMEM((K_CHUNKS, depth, hd), BF16),
                pltpu.VMEM((K_CHUNKS, depth, hd), BF16),
                pltpu.VMEM((RING, PER_GROUP, context, hd), BF16),
                pltpu.VMEM((RING, PER_GROUP, context, hd), BF16),
                pltpu.SMEM((batch,), jnp.int32),
                pltpu.SMEM((batch,), jnp.int32),
                pltpu.SemaphoreType.DMA((K_CHUNKS, 5)),
                pltpu.SemaphoreType.DMA((RING, PER_GROUP, context // BLOCK)),
                pltpu.SemaphoreType.DMA((RING, PER_GROUP, context // BLOCK)),
                pltpu.SemaphoreType.DMA((3,)),
            ],
            compiler_params=pltpu.CompilerParams(vmem_limit_bytes=32 * 2**20),
            name="project_and_attend_long",
        )(lengths, x, w_query, w_key, w_value, w_out, k_cache, v_cache)

        new_shape = (batch, kv_heads, hd)
        result = (sds((batch, width), BF16), sds(new_shape, BF16), sds(new_shape, BF16))
        held = pl.pallas_call(
            attend_short_and_reduce,
            out_shape=result,
            in_specs=[vmem] * 8 + [hbm] * 3,
            out_specs=[vmem] * 3,
            scratch_shapes=[
                pltpu.VMEM((batch, width), BF16),
                pltpu.VMEM((width, 2 * kv_width), BF16),
                pltpu.VMEM((batch, heads * hd), F32),
                pltpu.VMEM((8, batch, piece), F32),
                pltpu.VMEM((4, batch, piece), F32),
                pltpu.VMEM((2, batch, piece), F32),
                pltpu.VMEM((batch, piece), F32),
                pltpu.VMEM(new_shape, F32),
                pltpu.SemaphoreType.DMA((3,)),
                pltpu.SemaphoreType.DMA((6, len(CHUNKS))),
                pltpu.SemaphoreType.DMA((6, len(CHUNKS))),
            ],
            compiler_params=pltpu.CompilerParams(
                vmem_limit_bytes=40 * 2**20, collective_id=0, has_side_effects=True
            ),
            name="attend_short_and_reduce",
        )(*ahead, x, w_key, w_value)
        return pl.pallas_call(
            copy_out,
            out_shape=result,
            in_specs=[vmem] * 3,
            out_specs=[pl.BlockSpec(memory_space=pltpu.HBM)] * 3,
            scratch_shapes=[pltpu.SemaphoreType.DMA((3,))],
            compiler_params=pltpu.CompilerParams(vmem_limit_bytes=2**20),
            name="copy_out",
        )(*held)

    rows_spec = P("replica")
    return jax.shard_map(
        local_step,
        mesh=mesh,
        in_specs=(P("replica", None), P(None, "model"), P(), P(), P("model", None), rows_spec, rows_spec, rows_spec),
        out_specs=(rows_spec, rows_spec, rows_spec),
        check_vma=False,
    )
```

```python
import functools

import jax
import jax.numpy as jnp
from jax import lax
from jax.experimental import pallas as pl
from jax.experimental.pallas import tpu as pltpu
from jax.sharding import PartitionSpec as P

BF16 = jnp.bfloat16
F32 = jnp.float32
SHORT = 32
PER_GROUP = 6
RING = 3
BLOCK = 256
K_CHUNKS = 4
UNROLL = 8
KV_STEPS = 8
PARTS = ((0, 64), (64, 192))
CHUNKS = ((0, 32), (32, 32), (64, 32), (96, 32), (128, 32), (160, 32), (192, 32), (224, 16), (240, 16))
ATTEND, PROJECT, NEW = 6, 7, 8
ORDER = (
    (6, 0), (7, 0), (6, 1), (7, 1), (0, 0), (0, 1), (0, 2), (0, 3), (0, 4), (0, 5), (0, 6), (0, 7),
    (1, 0), (0, 8), (8, 0), (1, 1), (8, 1), (8, 2), (8, 3), (2, 0), (1, 2), (8, 4), (8, 5), (2, 1),
    (1, 3), (8, 6), (8, 7), (3, 0), (1, 4), (2, 2), (3, 1), (2, 3), (1, 5), (2, 4), (3, 2), (3, 3),
    (1, 6), (2, 5), (1, 7), (3, 4), (1, 8), (2, 6), (4, 0), (3, 5), (2, 7), (5, 0), (4, 1), (2, 8),
    (3, 6), (4, 2), (5, 1), (3, 7), (4, 3), (5, 2), (3, 8), (4, 4), (5, 3), (4, 5), (5, 4), (4, 6),
    (4, 7), (5, 5), (4, 8), (5, 6), (5, 7), (5, 8),
)
NT = (((1,), (1,)), ((), ()))


def project_and_attend_long(
    lens_hbm, x, wq, wk, wv, wo, kc, vc,
    q_out, k1_out, v1_out, ol_out, lv_out, ks_out, vs_out, wo_out,
    xbuf, wqbuf, wkbuf, wvbuf, kbuf, vbuf, ebuf, nbuf, tbuf, lens, idx, wsem, ksem, vsem, next_sem,
):
    me = lax.axis_index("model")
    batch = lv_out.shape[0]
    heads, _, hd = q_out.shape
    context = kc.shape[2]
    blocks = context // BLOCK
    scale = hd ** -0.5
    depth = xbuf.shape[2]

    def loads(i):
        rows = pl.ds(i * depth, depth)
        cols = pl.ds(pl.multiple_of(me * hd, hd), hd)
        return (
            pltpu.make_async_copy(x.at[:, rows], xbuf.at[i], wsem.at[i, 0]),
            pltpu.make_async_copy(wq.at[rows, :], wqbuf.at[i], wsem.at[i, 1]),
            pltpu.make_async_copy(wk.at[rows, cols], wkbuf.at[i], wsem.at[i, 2]),
            pltpu.make_async_copy(wv.at[rows, cols], wvbuf.at[i], wsem.at[i, 3]),
        )

    lens_load = pltpu.make_async_copy(lens_hbm, lens, wsem.at[0, 4])
    lens_load.start()
    for i in range(K_CHUNKS):
        for copy in loads(i):
            copy.start()
    vbuf[...] = jnp.zeros_like(vbuf)
    lens_load.wait()

    def scan(b, n):
        idx[n] = b
        return n + (lens[b] > SHORT).astype(jnp.int32)

    n_long = lax.fori_loop(0, batch, scan, jnp.int32(0), unroll=16)
    n_groups = (n_long + PER_GROUP - 1) // PER_GROUP

    def sequence(g, j):
        return idx[jnp.maximum(jnp.minimum(g * PER_GROUP + j, n_long - 1), 0)]

    def each_block(g, act):
        slot = lax.rem(g, RING)
        for j in range(PER_GROUP):
            b = sequence(g, j)
            length = lens[b]
            for t in range(blocks):
                rows = pl.ds(t * BLOCK, BLOCK)

                @pl.when(length > t * BLOCK)
                def _():
                    act(pltpu.make_async_copy(kc.at[b, me, rows, :], kbuf.at[slot, j, rows, :], ksem.at[slot, j, t]))
                    act(pltpu.make_async_copy(vc.at[b, me, rows, :], vbuf.at[slot, j, rows, :], vsem.at[slot, j, t]))

    for g in range(RING):
        @pl.when(g < n_groups)
        def _():
            each_block(jnp.int32(g), lambda copy: copy.start())

    ahead = (
        pltpu.make_async_copy(kc.at[:, me, pl.ds(0, SHORT), :], ks_out, next_sem.at[0]),
        pltpu.make_async_copy(vc.at[:, me, pl.ds(0, SHORT), :], vs_out, next_sem.at[1]),
        pltpu.make_async_copy(wo, wo_out, next_sem.at[2]),
    )
    def spread(b, carry):
        lv_out[pl.ds(b, 1), :] = jnp.full((1, hd), lens[b], jnp.int32)
        return carry

    lax.fori_loop(0, batch, spread, 0, unroll=8)

    for i in range(K_CHUNKS):
        for copy in loads(i):
            copy.wait()
        xs = xbuf[i]
        q_part = jnp.dot(xs, wqbuf[i], preferred_element_type=F32)
        k_part = jnp.dot(xs, wkbuf[i], preferred_element_type=F32)
        v_part = jnp.dot(xs, wvbuf[i], preferred_element_type=F32)
        for h in range(heads):
            piece = q_part[:, h * hd:(h + 1) * hd]
            q_out[h] = piece if i == 0 else q_out[h] + piece
        k1_out[...] = k_part if i == 0 else k1_out[...] + k_part
        v1_out[...] = v_part if i == 0 else v1_out[...] + v_part
    for copy in ahead:
        copy.start()

    q_out[...] = q_out[...].astype(BF16).astype(F32)
    k1_out[...] = k1_out[...].astype(BF16).astype(F32)
    v1_out[...] = v1_out[...].astype(BF16).astype(F32)

    def attend(g, carry):
        slot = lax.rem(g, RING)
        each_block(g, lambda copy: copy.wait())
        for j in range(PER_GROUP):
            b = sequence(g, j)
            length = lens[b]
            row = pl.ds(b, 1)
            q = jnp.concatenate([q_out[h, row, :] for h in range(heads)] * 2, axis=0)
            k1, v1 = k1_out[row, :], v1_out[row, :]
            s = lax.dot_general(q.astype(BF16), kbuf[slot, j], NT, preferred_element_type=F32) * scale
            s_new = jnp.sum(q * k1, axis=-1, keepdims=True) * scale
            s = jnp.where(lax.broadcasted_iota(jnp.int32, s.shape, 1) < length, s, -jnp.inf)
            m = jnp.maximum(jnp.max(s, axis=-1, keepdims=True), s_new)
            e = jnp.exp(s - m)
            e_new = jnp.exp(s_new - m)
            total = jnp.sum(e, axis=-1, keepdims=True) + e_new
            ebuf[j] = e.astype(BF16)
            nbuf[j] = e_new.astype(BF16).astype(F32) * v1
            tbuf[j] = jnp.broadcast_to(total, (8, hd))

        @pl.when(g < n_groups)
        def _():
            for j in range(PER_GROUP):
                row = pl.ds(sequence(g, j), 1)
                o = jnp.dot(ebuf[j], vbuf[slot, j], preferred_element_type=F32)
                o = (o + nbuf[j]) / tbuf[j]
                for h in range(heads):
                    ol_out[h, row, :] = o[h:h + 1, :]

        @pl.when(g + RING < n_groups)
        def _():
            each_block(g + RING, lambda copy: copy.start())

        return carry

    lax.fori_loop(0, n_groups, attend, 0)
    for copy in ahead:
        copy.wait()


def attend_short_and_reduce(
    q_ref, k1_ref, v1_ref, ol_ref, lv_ref, kbuf, vbuf, wobuf, x, wk, wv,
    y_out, kn_out, vn_out,
    xbuf, wkv, ebuf, nbuf, tbuf, obuf, part, got_core, got_one, got_two, kvbuf,
    load_sem, send_sem, recv_sem,
):
    me = lax.axis_index("model")
    core = me % 2
    px = (me // 2) % 2
    py = me // 4
    flip_x = me + 2 - 4 * px
    flip_y = me + 4 - 8 * py
    other_core = 1 - core
    partner = me + 1 - 2 * core
    near_one = other_core * flip_x + core * flip_y
    near_two = other_core * flip_y + core * flip_x
    a = other_core * px + core * py
    b = other_core * py + core * px
    base = 4 * core
    mine = base + 2 * a + b
    heads, batch, hd = q_ref.shape
    width = part.shape[2]
    kv_width = wkv.shape[1] // 2
    kv_heads = kv_width // hd
    slice_heads = 2 * kv_heads // KV_STEPS
    scale = hd ** -0.5

    loads = (
        pltpu.make_async_copy(x, xbuf, load_sem.at[0]),
        pltpu.make_async_copy(wk, wkv.at[:, pl.ds(0, kv_width)], load_sem.at[1]),
        pltpu.make_async_copy(wv, wkv.at[:, pl.ds(kv_width, kv_width)], load_sem.at[2]),
    )
    for copy in loads:
        copy.start()

    barrier = pltpu.get_barrier_semaphore()
    for other in (partner, near_one, near_two):
        pl.semaphore_signal(barrier, inc=1, device_id={"model": other}, device_id_type=pl.DeviceIdType.MESH)

    def rows_of(r):
        first, count = CHUNKS[r]
        return pl.ds(first, count)

    def cols_of(f, count):
        return pl.ds(pl.multiple_of(f * width, width), count * width)

    def send(stage, r):
        rows = rows_of(r)
        if stage == 0:
            src, dst, other = part.at[pl.ds(4 * other_core, 4), rows], got_core.at[:, rows], partner
        elif stage == 1:
            src, dst, other = part.at[pl.ds(base + 2 * (1 - a), 2), rows], got_one.at[:, rows], near_one
        elif stage == 2:
            src, dst, other = part.at[base + 2 * a + 1 - b, rows], got_two.at[rows], near_two
        elif stage == 3:
            src = dst = y_out.at[rows, cols_of(mine, 1)]
            other = near_two
        elif stage == 4:
            src = dst = y_out.at[rows, cols_of(base + 2 * a, 2)]
            other = near_one
        else:
            src = dst = y_out.at[rows, cols_of(base, 4)]
            other = partner
        return pltpu.make_async_remote_copy(
            src_ref=src, dst_ref=dst, send_sem=send_sem.at[stage, r], recv_sem=recv_sem.at[stage, r],
            device_id={"model": other}, device_id_type=pl.DeviceIdType.MESH,
        )

    def advance(stage, r):
        rows = rows_of(r)
        send(stage, r).wait()
        if stage == 0:
            part[pl.ds(base, 4), rows] += got_core[:, rows]
        elif stage == 1:
            part[pl.ds(base + 2 * a, 2), rows] += got_one[:, rows]
        elif stage == 2:
            total = part[mine, rows] + got_two[rows]
            total = total + xbuf[rows, cols_of(mine, 1)].astype(F32)
            y_out[rows, cols_of(mine, 1)] = total.astype(BF16)
        if stage < 5:
            send(stage + 1, r).start()

    def weigh(group):
        rows = pl.ds(pl.multiple_of(group * 8, 8), 8)
        q = jnp.concatenate([q_ref[h, rows, :] for h in range(heads)], axis=0)
        k1 = jnp.concatenate([k1_ref[rows, :]] * heads, axis=0)
        v1 = jnp.concatenate([v1_ref[rows, :]] * heads, axis=0)
        lens = jnp.concatenate([lv_ref[rows, :]] * heads, axis=0)
        k = kbuf[rows].reshape(8 * SHORT, hd)
        s = lax.dot_general(q.astype(BF16), k, NT, preferred_element_type=F32) * scale
        s_new = jnp.sum(q * k1, axis=-1, keepdims=True) * scale
        lane = lax.broadcasted_iota(jnp.int32, s.shape, 1)
        line = lax.broadcasted_iota(jnp.int32, s.shape, 0)
        slot = lane - (line % 8) * SHORT
        wide = jnp.concatenate([lens] * (s.shape[1] // hd), axis=1)
        s = jnp.where((slot >= 0) & (slot < jnp.minimum(wide, SHORT)), s, -jnp.inf)
        m = jnp.maximum(jnp.max(s, axis=-1, keepdims=True), s_new)
        e = jnp.exp(s - m)
        e_new = jnp.exp(s_new - m)
        total = jnp.sum(e, axis=-1, keepdims=True) + e_new
        ebuf[group] = e.astype(BF16)
        nbuf[group] = e_new.astype(BF16).astype(F32) * v1
        tbuf[group] = jnp.broadcast_to(total, (8 * heads, hd))

    def gather(group):
        rows = pl.ds(pl.multiple_of(group * 8, 8), 8)
        v = vbuf[rows].reshape(8 * SHORT, hd)
        o = jnp.dot(ebuf[group], v, preferred_element_type=F32)
        o = (o + nbuf[group]) / tbuf[group]
        long = lv_ref[rows, :] > SHORT
        for h in range(heads):
            obuf[rows, pl.ds(h * hd, hd)] = jnp.where(long, ol_ref[h, rows, :], o[h * 8:(h + 1) * 8])

    def attend(first, count):
        for act in (weigh, gather):
            def body(i, carry):
                for g in range(UNROLL):
                    act(first // 8 + i * UNROLL + g)
                return carry

            lax.fori_loop(0, count // 8 // UNROLL, body, 0)

    def project_out(first, count):
        rows = pl.ds(first, count)
        o_rows = obuf[rows, :].astype(BF16)
        for f in range(8):
            part[f, rows] = jnp.dot(o_rows, wobuf[:, f * width:(f + 1) * width], preferred_element_type=F32)

    def new_rows(t):
        if t == 0:
            loads[0].wait()
            loads[1].wait()
            loads[2].wait()
        cols = pl.ds(t * slice_heads * hd, slice_heads * hd)
        fresh = jnp.dot(xbuf[...], wkv[:, cols], preferred_element_type=F32)
        for h in range(slice_heads):
            kvbuf[:, (t * slice_heads + h) % kv_heads, :] = fresh[:, h * hd:(h + 1) * hd]
        if t == KV_STEPS // 2 - 1:
            kn_out[...] = kvbuf[...].astype(BF16)
        if t == KV_STEPS - 1:
            vn_out[...] = kvbuf[...].astype(BF16)

    for op, i in ORDER:
        if op == ATTEND:
            attend(*PARTS[i])
        elif op == PROJECT:
            project_out(*PARTS[i])
            if i == 0:
                pl.semaphore_wait(barrier, 3)
            for r, (first, _) in enumerate(CHUNKS):
                if PARTS[i][0] <= first < PARTS[i][0] + PARTS[i][1]:
                    send(0, r).start()
        elif op == NEW:
            new_rows(i)
        else:
            advance(op, i)


def copy_out(y, kn, vn, y_out, kn_out, vn_out, sem):
    copies = [
        pltpu.make_async_copy(src, dst, sem.at[i])
        for i, (src, dst) in enumerate(((y, y_out), (kn, kn_out), (vn, vn_out)))
    ]
    for copy in copies:
        copy.start()
    for copy in copies:
        copy.wait()


def solution(mesh):
    def local_step(x, w_query, w_key, w_value, w_out, k_cache, v_cache, lengths):
        batch, width = x.shape
        kv_heads, context, hd = k_cache.shape[1:]
        heads = w_query.shape[1] // hd
        kv_width = kv_heads * hd
        depth = width // K_CHUNKS
        piece = width // 8
        vmem = pl.BlockSpec(memory_space=pltpu.VMEM)
        hbm = pl.BlockSpec(memory_space=pltpu.HBM)
        sds = jax.ShapeDtypeStruct
        x, w_query, w_key, w_value, w_out, k_cache, v_cache, lengths = (
            pltpu.with_memory_space_constraint(array, pltpu.HBM)
            for array in (x, w_query, w_key, w_value, w_out, k_cache, v_cache, lengths)
        )

        ahead = pl.pallas_call(
            project_and_attend_long,
            out_shape=(
                sds((heads, batch, hd), F32), sds((batch, hd), F32), sds((batch, hd), F32),
                sds((heads, batch, hd), F32), sds((batch, hd), jnp.int32),
                sds((batch, SHORT, hd), BF16), sds((batch, SHORT, hd), BF16), sds((heads * hd, width), BF16),
            ),
            in_specs=[hbm] * 8,
            out_specs=[vmem] * 8,
            scratch_shapes=[
                pltpu.VMEM((K_CHUNKS, batch, depth), BF16),
                pltpu.VMEM((K_CHUNKS, depth, heads * hd), BF16),
                pltpu.VMEM((K_CHUNKS, depth, hd), BF16),
                pltpu.VMEM((K_CHUNKS, depth, hd), BF16),
                pltpu.VMEM((RING, PER_GROUP, context, hd), BF16),
                pltpu.VMEM((RING, PER_GROUP, context, hd), BF16),
                pltpu.VMEM((PER_GROUP, 8, context), BF16),
                pltpu.VMEM((PER_GROUP, 8, hd), F32),
                pltpu.VMEM((PER_GROUP, 8, hd), F32),
                pltpu.SMEM((batch,), jnp.int32),
                pltpu.SMEM((batch,), jnp.int32),
                pltpu.SemaphoreType.DMA((K_CHUNKS, 5)),
                pltpu.SemaphoreType.DMA((RING, PER_GROUP, context // BLOCK)),
                pltpu.SemaphoreType.DMA((RING, PER_GROUP, context // BLOCK)),
                pltpu.SemaphoreType.DMA((3,)),
            ],
            compiler_params=pltpu.CompilerParams(vmem_limit_bytes=28 * 2**20),
            name="project_and_attend_long",
        )(lengths, x, w_query, w_key, w_value, w_out, k_cache, v_cache)

        new_shape = (batch, kv_heads, hd)
        result = (sds((batch, width), BF16), sds(new_shape, BF16), sds(new_shape, BF16))
        held = pl.pallas_call(
            attend_short_and_reduce,
            out_shape=result,
            in_specs=[vmem] * 8 + [hbm] * 3,
            out_specs=[vmem] * 3,
            scratch_shapes=[
                pltpu.VMEM((batch, width), BF16),
                pltpu.VMEM((width, 2 * kv_width), BF16),
                pltpu.VMEM((batch // 8, 8 * heads, 8 * SHORT), BF16),
                pltpu.VMEM((batch // 8, 8 * heads, hd), F32),
                pltpu.VMEM((batch // 8, 8 * heads, hd), F32),
                pltpu.VMEM((batch, heads * hd), F32),
                pltpu.VMEM((8, batch, piece), F32),
                pltpu.VMEM((4, batch, piece), F32),
                pltpu.VMEM((2, batch, piece), F32),
                pltpu.VMEM((batch, piece), F32),
                pltpu.VMEM(new_shape, F32),
                pltpu.SemaphoreType.DMA((3,)),
                pltpu.SemaphoreType.DMA((6, len(CHUNKS))),
                pltpu.SemaphoreType.DMA((6, len(CHUNKS))),
            ],
            compiler_params=pltpu.CompilerParams(
                vmem_limit_bytes=40 * 2**20, collective_id=0, has_side_effects=True
            ),
            name="attend_short_and_reduce",
        )(*ahead, x, w_key, w_value)
        return pl.pallas_call(
            copy_out,
            out_shape=result,
            in_specs=[vmem] * 3,
            out_specs=[pl.BlockSpec(memory_space=pltpu.HBM)] * 3,
            scratch_shapes=[pltpu.SemaphoreType.DMA((3,))],
            compiler_params=pltpu.CompilerParams(vmem_limit_bytes=2**20),
            name="copy_out",
        )(*held)

    rows_spec = P("replica")
    return jax.shard_map(
        local_step,
        mesh=mesh,
        in_specs=(P("replica", None), P(None, "model"), P(), P(), P("model", None), rows_spec, rows_spec, rows_spec),
        out_specs=(rows_spec, rows_spec, rows_spec),
        check_vma=False,
    )
```

```python
import functools

import jax
import jax.numpy as jnp
from jax import lax
from jax.experimental import pallas as pl
from jax.experimental.pallas import tpu as pltpu
from jax.sharding import PartitionSpec as P

BF16 = jnp.bfloat16
F32 = jnp.float32
SHORT = 32
PER_GROUP = 6
RING = 3
BLOCK = 256
K_CHUNKS = 4
UNROLL = 8
KV_STEPS = 8
PARTS = ((0, 64), (64, 192))
CHUNKS = ((0, 64), (64, 48), (112, 48), (160, 48), (208, 32), (240, 16))
DIRECT_SUM = ()
DIRECT_SHARE = (4, 5)
ATTEND, PROJECT, NEW = 6, 7, 8
ORDER = (
    (6, 0), (7, 0), (6, 1), (0, 0), (7, 1), (0, 1), (0, 2), (0, 3), (0, 4), (0, 5), (8, 0), (1, 0),
    (8, 1), (8, 2), (8, 3), (1, 1), (8, 4), (8, 5), (8, 6), (8, 7), (2, 0), (1, 2), (2, 1), (3, 0),
    (1, 3), (2, 2), (3, 1), (1, 4), (1, 5), (2, 3), (3, 2), (4, 0), (2, 4), (2, 5), (5, 0), (3, 3),
    (4, 1), (3, 4), (5, 1), (3, 5), (4, 2), (5, 2), (4, 3), (4, 4), (4, 5), (5, 3), (5, 4), (5, 5),
)
NT = (((1,), (1,)), ((), ()))


def project_and_attend_long(
    lens_hbm, x, wq, wk, wv, wo, kc, vc,
    q_out, k1_out, v1_out, ol_out, lv_out, ks_out, vs_out, wo_out,
    xbuf, wqbuf, wkbuf, wvbuf, kbuf, vbuf, ebuf, nbuf, tbuf, lens, idx, wsem, ksem, vsem, next_sem,
):
    me = lax.axis_index("model")
    batch = lv_out.shape[0]
    heads, _, hd = q_out.shape
    context = kc.shape[2]
    blocks = context // BLOCK
    scale = hd ** -0.5
    depth = xbuf.shape[2]

    def loads(i):
        rows = pl.ds(i * depth, depth)
        cols = pl.ds(pl.multiple_of(me * hd, hd), hd)
        return (
            pltpu.make_async_copy(x.at[:, rows], xbuf.at[i], wsem.at[i, 0]),
            pltpu.make_async_copy(wq.at[rows, :], wqbuf.at[i], wsem.at[i, 1]),
            pltpu.make_async_copy(wk.at[rows, cols], wkbuf.at[i], wsem.at[i, 2]),
            pltpu.make_async_copy(wv.at[rows, cols], wvbuf.at[i], wsem.at[i, 3]),
        )

    lens_load = pltpu.make_async_copy(lens_hbm, lens, wsem.at[0, 4])
    lens_load.start()
    for i in range(K_CHUNKS):
        for copy in loads(i):
            copy.start()
    vbuf[...] = jnp.zeros_like(vbuf)
    lens_load.wait()

    def scan(b, n):
        idx[n] = b
        return n + (lens[b] > SHORT).astype(jnp.int32)

    n_long = lax.fori_loop(0, batch, scan, jnp.int32(0), unroll=16)
    n_groups = (n_long + PER_GROUP - 1) // PER_GROUP

    def sequence(g, j):
        return idx[jnp.maximum(jnp.minimum(g * PER_GROUP + j, n_long - 1), 0)]

    def each_block(g, act):
        slot = lax.rem(g, RING)
        for j in range(PER_GROUP):
            b = sequence(g, j)
            length = lens[b]
            for t in range(blocks):
                rows = pl.ds(t * BLOCK, BLOCK)

                @pl.when(length > t * BLOCK)
                def _():
                    act(pltpu.make_async_copy(kc.at[b, me, rows, :], kbuf.at[slot, j, rows, :], ksem.at[slot, j, t]))
                    act(pltpu.make_async_copy(vc.at[b, me, rows, :], vbuf.at[slot, j, rows, :], vsem.at[slot, j, t]))

    for g in range(RING):
        @pl.when(g < n_groups)
        def _():
            each_block(jnp.int32(g), lambda copy: copy.start())

    ahead = (
        pltpu.make_async_copy(kc.at[:, me, pl.ds(0, SHORT), :], ks_out, next_sem.at[0]),
        pltpu.make_async_copy(vc.at[:, me, pl.ds(0, SHORT), :], vs_out, next_sem.at[1]),
        pltpu.make_async_copy(wo, wo_out, next_sem.at[2]),
    )
    def spread(b, carry):
        lv_out[pl.ds(b, 1), :] = jnp.full((1, hd), lens[b], jnp.int32)
        return carry

    lax.fori_loop(0, batch, spread, 0, unroll=8)

    for i in range(K_CHUNKS):
        for copy in loads(i):
            copy.wait()
        xs = xbuf[i]
        q_part = jnp.dot(xs, wqbuf[i], preferred_element_type=F32)
        k_part = jnp.dot(xs, wkbuf[i], preferred_element_type=F32)
        v_part = jnp.dot(xs, wvbuf[i], preferred_element_type=F32)
        for h in range(heads):
            piece = q_part[:, h * hd:(h + 1) * hd]
            q_out[h] = piece if i == 0 else q_out[h] + piece
        k1_out[...] = k_part if i == 0 else k1_out[...] + k_part
        v1_out[...] = v_part if i == 0 else v1_out[...] + v_part
    for copy in ahead:
        copy.start()

    q_out[...] = q_out[...].astype(BF16).astype(F32)
    k1_out[...] = k1_out[...].astype(BF16).astype(F32)
    v1_out[...] = v1_out[...].astype(BF16).astype(F32)

    def attend(g, carry):
        slot = lax.rem(g, RING)
        each_block(g, lambda copy: copy.wait())
        for j in range(PER_GROUP):
            b = sequence(g, j)
            length = lens[b]
            row = pl.ds(b, 1)
            q = jnp.concatenate([q_out[h, row, :] for h in range(heads)] * 2, axis=0)
            k1, v1 = k1_out[row, :], v1_out[row, :]
            s = lax.dot_general(q.astype(BF16), kbuf[slot, j], NT, preferred_element_type=F32) * scale
            s_new = jnp.sum(q * k1, axis=-1, keepdims=True) * scale
            s = jnp.where(lax.broadcasted_iota(jnp.int32, s.shape, 1) < length, s, -jnp.inf)
            m = jnp.maximum(jnp.max(s, axis=-1, keepdims=True), s_new)
            e = jnp.exp(s - m)
            e_new = jnp.exp(s_new - m)
            total = jnp.sum(e, axis=-1, keepdims=True) + e_new
            ebuf[j] = e.astype(BF16)
            nbuf[j] = e_new.astype(BF16).astype(F32) * v1
            tbuf[j] = jnp.broadcast_to(total, (8, hd))

        @pl.when(g < n_groups)
        def _():
            for j in range(PER_GROUP):
                row = pl.ds(sequence(g, j), 1)
                o = jnp.dot(ebuf[j], vbuf[slot, j], preferred_element_type=F32)
                o = (o + nbuf[j]) / tbuf[j]
                for h in range(heads):
                    ol_out[h, row, :] = o[h:h + 1, :]

        @pl.when(g + RING < n_groups)
        def _():
            each_block(g + RING, lambda copy: copy.start())

        return carry

    lax.fori_loop(0, n_groups, attend, 0)
    for copy in ahead:
        copy.wait()


def attend_short_and_reduce(
    q_ref, k1_ref, v1_ref, ol_ref, lv_ref, kbuf, vbuf, wobuf, x, wk, wv,
    y_out, kn_out, vn_out,
    xbuf, wkv, ebuf, nbuf, tbuf, obuf, part, got_core, got_one, got_two, kvbuf,
    load_sem, send_sem, recv_sem,
):
    me = lax.axis_index("model")
    core = me % 2
    px = (me // 2) % 2
    py = me // 4
    flip_x = me + 2 - 4 * px
    flip_y = me + 4 - 8 * py
    other_core = 1 - core
    partner = me + 1 - 2 * core
    across = flip_x + 4 - 8 * py
    near_one = other_core * flip_x + core * flip_y
    near_two = other_core * flip_y + core * flip_x
    a = other_core * px + core * py
    b = other_core * py + core * px
    base = 4 * core
    mine = base + 2 * a + b
    heads, batch, hd = q_ref.shape
    width = part.shape[2]
    kv_width = wkv.shape[1] // 2
    kv_heads = kv_width // hd
    slice_heads = 2 * kv_heads // KV_STEPS
    scale = hd ** -0.5

    loads = (
        pltpu.make_async_copy(x, xbuf, load_sem.at[0]),
        pltpu.make_async_copy(wk, wkv.at[:, pl.ds(0, kv_width)], load_sem.at[1]),
        pltpu.make_async_copy(wv, wkv.at[:, pl.ds(kv_width, kv_width)], load_sem.at[2]),
    )
    for copy in loads:
        copy.start()

    barrier = pltpu.get_barrier_semaphore()
    for other in (partner, near_one, near_two, across):
        pl.semaphore_signal(barrier, inc=1, device_id={"model": other}, device_id_type=pl.DeviceIdType.MESH)

    def rows_of(r):
        first, count = CHUNKS[r]
        return pl.ds(first, count)

    def cols_of(f, count):
        return pl.ds(pl.multiple_of(f * width, width), count * width)

    def send(stage, r):
        rows = rows_of(r)
        if stage == 0:
            src, dst, other = part.at[pl.ds(4 * other_core, 4), rows], got_core.at[:, rows], partner
        elif stage == 1 and r in DIRECT_SUM:
            src, dst, other = part.at[base + 2 * (1 - a) + b, rows], got_one.at[0, rows], near_one
        elif stage == 1:
            src, dst, other = part.at[pl.ds(base + 2 * (1 - a), 2), rows], got_one.at[:, rows], near_one
        elif stage == 2:
            src, dst, other = part.at[base + 2 * a + 1 - b, rows], got_two.at[rows], near_two
        elif stage == 6:
            src, dst, other = part.at[base + 2 * (1 - a) + 1 - b, rows], got_one.at[1, rows], across
        elif stage == 3:
            src = dst = y_out.at[rows, cols_of(mine, 1)]
            other = near_two
        elif stage == 7 or (stage == 4 and r in DIRECT_SHARE):
            src = dst = y_out.at[rows, cols_of(mine, 1)]
            other = across if stage == 7 else near_one
        elif stage == 4:
            src = dst = y_out.at[rows, cols_of(base + 2 * a, 2)]
            other = near_one
        else:
            src = dst = y_out.at[rows, cols_of(base, 4)]
            other = partner
        return pltpu.make_async_remote_copy(
            src_ref=src, dst_ref=dst, send_sem=send_sem.at[stage, r], recv_sem=recv_sem.at[stage, r],
            device_id={"model": other}, device_id_type=pl.DeviceIdType.MESH,
        )

    def advance(stage, r):
        rows = rows_of(r)
        send(stage, r).wait()
        following = (stage + 1,) if stage < 5 else ()
        if stage == 0:
            part[pl.ds(base, 4), rows] += got_core[:, rows]
            if r in DIRECT_SUM:
                following = (6, 1, 2)
        elif stage == 1:
            if r in DIRECT_SUM:
                following = ()
            else:
                part[pl.ds(base + 2 * a, 2), rows] += got_one[:, rows]
        elif stage == 2:
            total = part[mine, rows] + got_two[rows]
            if r in DIRECT_SUM:
                send(6, r).wait()
                total = total + (got_one[0, rows] + got_one[1, rows])
            total = total + xbuf[rows, cols_of(mine, 1)].astype(F32)
            y_out[rows, cols_of(mine, 1)] = total.astype(BF16)
            if r in DIRECT_SHARE:
                following = (7, 3, 4)
        elif stage == 3 and r in DIRECT_SHARE:
            following = ()
        elif stage == 4 and r in DIRECT_SHARE:
            send(7, r).wait()
        for later in following:
            send(later, r).start()

    def weigh(group):
        rows = pl.ds(pl.multiple_of(group * 8, 8), 8)
        q = jnp.concatenate([q_ref[h, rows, :] for h in range(heads)], axis=0)
        k1 = jnp.concatenate([k1_ref[rows, :]] * heads, axis=0)
        v1 = jnp.concatenate([v1_ref[rows, :]] * heads, axis=0)
        lens = jnp.concatenate([lv_ref[rows, :]] * heads, axis=0)
        k = kbuf[rows].reshape(8 * SHORT, hd)
        s = lax.dot_general(q.astype(BF16), k, NT, preferred_element_type=F32) * scale
        s_new = jnp.sum(q * k1, axis=-1, keepdims=True) * scale
        lane = lax.broadcasted_iota(jnp.int32, s.shape, 1)
        line = lax.broadcasted_iota(jnp.int32, s.shape, 0)
        slot = lane - (line % 8) * SHORT
        wide = jnp.concatenate([lens] * (s.shape[1] // hd), axis=1)
        s = jnp.where((slot >= 0) & (slot < jnp.minimum(wide, SHORT)), s, -jnp.inf)
        m = jnp.maximum(jnp.max(s, axis=-1, keepdims=True), s_new)
        e = jnp.exp(s - m)
        e_new = jnp.exp(s_new - m)
        total = jnp.sum(e, axis=-1, keepdims=True) + e_new
        ebuf[group] = e.astype(BF16)
        nbuf[group] = e_new.astype(BF16).astype(F32) * v1
        tbuf[group] = jnp.broadcast_to(total, (8 * heads, hd))

    def gather(group):
        rows = pl.ds(pl.multiple_of(group * 8, 8), 8)
        v = vbuf[rows].reshape(8 * SHORT, hd)
        o = jnp.dot(ebuf[group], v, preferred_element_type=F32)
        o = (o + nbuf[group]) / tbuf[group]
        long = lv_ref[rows, :] > SHORT
        for h in range(heads):
            obuf[rows, pl.ds(h * hd, hd)] = jnp.where(long, ol_ref[h, rows, :], o[h * 8:(h + 1) * 8])

    def attend(first, count):
        for act in (weigh, gather):
            def body(i, carry):
                for g in range(UNROLL):
                    act(first // 8 + i * UNROLL + g)
                return carry

            lax.fori_loop(0, count // 8 // UNROLL, body, 0)

    def project_out(first, count):
        rows = pl.ds(first, count)
        o_rows = obuf[rows, :].astype(BF16)
        for f in range(8):
            part[f, rows] = jnp.dot(o_rows, wobuf[:, f * width:(f + 1) * width], preferred_element_type=F32)

    def new_rows(t):
        if t == 0:
            loads[0].wait()
            loads[1].wait()
            loads[2].wait()
        cols = pl.ds(t * slice_heads * hd, slice_heads * hd)
        fresh = jnp.dot(xbuf[...], wkv[:, cols], preferred_element_type=F32)
        for h in range(slice_heads):
            kvbuf[:, (t * slice_heads + h) % kv_heads, :] = fresh[:, h * hd:(h + 1) * hd]
        if t == KV_STEPS // 2 - 1:
            kn_out[...] = kvbuf[...].astype(BF16)
        if t == KV_STEPS - 1:
            vn_out[...] = kvbuf[...].astype(BF16)

    for op, i in ORDER:
        if op == ATTEND:
            attend(*PARTS[i])
        elif op == PROJECT:
            project_out(*PARTS[i])
            if i == 0:
                pl.semaphore_wait(barrier, 4)
            for r, (first, _) in enumerate(CHUNKS):
                if PARTS[i][0] <= first < PARTS[i][0] + PARTS[i][1]:
                    send(0, r).start()
        elif op == NEW:
            new_rows(i)
        else:
            advance(op, i)


def copy_out(y, kn, vn, y_out, kn_out, vn_out, sem):
    copies = [
        pltpu.make_async_copy(src, dst, sem.at[i])
        for i, (src, dst) in enumerate(((y, y_out), (kn, kn_out), (vn, vn_out)))
    ]
    for copy in copies:
        copy.start()
    for copy in copies:
        copy.wait()


def solution(mesh):
    def local_step(x, w_query, w_key, w_value, w_out, k_cache, v_cache, lengths):
        batch, width = x.shape
        kv_heads, context, hd = k_cache.shape[1:]
        heads = w_query.shape[1] // hd
        kv_width = kv_heads * hd
        depth = width // K_CHUNKS
        piece = width // 8
        vmem = pl.BlockSpec(memory_space=pltpu.VMEM)
        hbm = pl.BlockSpec(memory_space=pltpu.HBM)
        sds = jax.ShapeDtypeStruct
        x, w_query, w_key, w_value, w_out, k_cache, v_cache, lengths = (
            pltpu.with_memory_space_constraint(array, pltpu.HBM)
            for array in (x, w_query, w_key, w_value, w_out, k_cache, v_cache, lengths)
        )

        ahead = pl.pallas_call(
            project_and_attend_long,
            out_shape=(
                sds((heads, batch, hd), F32), sds((batch, hd), F32), sds((batch, hd), F32),
                sds((heads, batch, hd), F32), sds((batch, hd), jnp.int32),
                sds((batch, SHORT, hd), BF16), sds((batch, SHORT, hd), BF16), sds((heads * hd, width), BF16),
            ),
            in_specs=[hbm] * 8,
            out_specs=[vmem] * 8,
            scratch_shapes=[
                pltpu.VMEM((K_CHUNKS, batch, depth), BF16),
                pltpu.VMEM((K_CHUNKS, depth, heads * hd), BF16),
                pltpu.VMEM((K_CHUNKS, depth, hd), BF16),
                pltpu.VMEM((K_CHUNKS, depth, hd), BF16),
                pltpu.VMEM((RING, PER_GROUP, context, hd), BF16),
                pltpu.VMEM((RING, PER_GROUP, context, hd), BF16),
                pltpu.VMEM((PER_GROUP, 8, context), BF16),
                pltpu.VMEM((PER_GROUP, 8, hd), F32),
                pltpu.VMEM((PER_GROUP, 8, hd), F32),
                pltpu.SMEM((batch,), jnp.int32),
                pltpu.SMEM((batch,), jnp.int32),
                pltpu.SemaphoreType.DMA((K_CHUNKS, 5)),
                pltpu.SemaphoreType.DMA((RING, PER_GROUP, context // BLOCK)),
                pltpu.SemaphoreType.DMA((RING, PER_GROUP, context // BLOCK)),
                pltpu.SemaphoreType.DMA((3,)),
            ],
            compiler_params=pltpu.CompilerParams(vmem_limit_bytes=28 * 2**20),
            name="project_and_attend_long",
        )(lengths, x, w_query, w_key, w_value, w_out, k_cache, v_cache)

        new_shape = (batch, kv_heads, hd)
        result = (sds((batch, width), BF16), sds(new_shape, BF16), sds(new_shape, BF16))
        held = pl.pallas_call(
            attend_short_and_reduce,
            out_shape=result,
            in_specs=[vmem] * 8 + [hbm] * 3,
            out_specs=[vmem] * 3,
            scratch_shapes=[
                pltpu.VMEM((batch, width), BF16),
                pltpu.VMEM((width, 2 * kv_width), BF16),
                pltpu.VMEM((batch // 8, 8 * heads, 8 * SHORT), BF16),
                pltpu.VMEM((batch // 8, 8 * heads, hd), F32),
                pltpu.VMEM((batch // 8, 8 * heads, hd), F32),
                pltpu.VMEM((batch, heads * hd), F32),
                pltpu.VMEM((8, batch, piece), F32),
                pltpu.VMEM((4, batch, piece), F32),
                pltpu.VMEM((2, batch, piece), F32),
                pltpu.VMEM((batch, piece), F32),
                pltpu.VMEM(new_shape, F32),
                pltpu.SemaphoreType.DMA((3,)),
                pltpu.SemaphoreType.DMA((8, len(CHUNKS))),
                pltpu.SemaphoreType.DMA((8, len(CHUNKS))),
            ],
            compiler_params=pltpu.CompilerParams(
                vmem_limit_bytes=40 * 2**20, collective_id=0, has_side_effects=True
            ),
            name="attend_short_and_reduce",
        )(*ahead, x, w_key, w_value)
        return pl.pallas_call(
            copy_out,
            out_shape=result,
            in_specs=[vmem] * 3,
            out_specs=[pl.BlockSpec(memory_space=pltpu.HBM)] * 3,
            scratch_shapes=[pltpu.SemaphoreType.DMA((3,))],
            compiler_params=pltpu.CompilerParams(vmem_limit_bytes=2**20),
            name="copy_out",
        )(*held)

    rows_spec = P("replica")
    return jax.shard_map(
        local_step,
        mesh=mesh,
        in_specs=(P("replica", None), P(None, "model"), P(), P(), P("model", None), rows_spec, rows_spec, rows_spec),
        out_specs=(rows_spec, rows_spec, rows_spec),
        check_vma=False,
    )
```

```python
import functools

import jax
import jax.numpy as jnp
from jax import lax
from jax.experimental import pallas as pl
from jax.experimental.pallas import tpu as pltpu
from jax.sharding import PartitionSpec as P

BF16 = jnp.bfloat16
F32 = jnp.float32
SHORT = 32
PER_GROUP = 6
RING = 3
BLOCK = 256
K_CHUNKS = 2
UNROLL = 8
KV_STEPS = 8
PARTS = ((0, 64), (64, 192))
CHUNKS = ((0, 64), (64, 48), (112, 48), (160, 48), (208, 32), (240, 16))
DIRECT_SUM = ()
DIRECT_SHARE = (3, 4, 5)
ATTEND, PROJECT, NEW = 6, 7, 8
ORDER = (
    (6, 0), (7, 0), (6, 1), (0, 0), (7, 1), (0, 1), (0, 2), (0, 3), (0, 4), (0, 5), (8, 0), (1, 0),
    (8, 1), (8, 2), (8, 3), (1, 1), (8, 4), (8, 5), (8, 6), (8, 7), (2, 0), (1, 2), (2, 1), (3, 0),
    (1, 3), (2, 2), (3, 1), (1, 4), (1, 5), (2, 3), (3, 2), (4, 0), (2, 4), (2, 5), (5, 0), (3, 3),
    (4, 1), (3, 4), (5, 1), (3, 5), (4, 2), (5, 2), (4, 3), (4, 4), (4, 5), (5, 3), (5, 4), (5, 5),
)
NT = (((1,), (1,)), ((), ()))


def project_and_attend_long(
    lens_hbm, x, wq, wk, wv, wo, kc, vc,
    q_out, k1_out, v1_out, ol_out, lv_out, ks_out, vs_out, wo_out,
    xbuf, wqbuf, wkbuf, wvbuf, kbuf, vbuf, ebuf, nbuf, tbuf, lens, idx, wsem, ksem, vsem, next_sem,
):
    me = lax.axis_index("model")
    batch = lv_out.shape[0]
    heads, _, hd = q_out.shape
    context = kc.shape[2]
    blocks = context // BLOCK
    scale = hd ** -0.5
    depth = xbuf.shape[2]

    def loads(i):
        rows = pl.ds(i * depth, depth)
        cols = pl.ds(pl.multiple_of(me * hd, hd), hd)
        return (
            pltpu.make_async_copy(x.at[:, rows], xbuf.at[i], wsem.at[i, 0]),
            pltpu.make_async_copy(wq.at[rows, :], wqbuf.at[i], wsem.at[i, 1]),
            pltpu.make_async_copy(wk.at[rows, cols], wkbuf.at[i], wsem.at[i, 2]),
            pltpu.make_async_copy(wv.at[rows, cols], wvbuf.at[i], wsem.at[i, 3]),
        )

    lens_load = pltpu.make_async_copy(lens_hbm, lens, wsem.at[0, 4])
    lens_load.start()
    for i in range(K_CHUNKS):
        for copy in loads(i):
            copy.start()
    vbuf[...] = jnp.zeros_like(vbuf)
    lens_load.wait()

    def scan(b, n):
        idx[n] = b
        return n + (lens[b] > SHORT).astype(jnp.int32)

    n_long = lax.fori_loop(0, batch, scan, jnp.int32(0), unroll=16)
    n_groups = (n_long + PER_GROUP - 1) // PER_GROUP

    def sequence(g, j):
        return idx[jnp.maximum(jnp.minimum(g * PER_GROUP + j, n_long - 1), 0)]

    def each_block(g, act):
        slot = lax.rem(g, RING)
        for j in range(PER_GROUP):
            b = sequence(g, j)
            length = lens[b]
            for t in range(blocks):
                rows = pl.ds(t * BLOCK, BLOCK)

                @pl.when(length > t * BLOCK)
                def _():
                    act(pltpu.make_async_copy(kc.at[b, me, rows, :], kbuf.at[slot, j, rows, :], ksem.at[slot, j, t]))
                    act(pltpu.make_async_copy(vc.at[b, me, rows, :], vbuf.at[slot, j, rows, :], vsem.at[slot, j, t]))

    for g in range(RING):
        @pl.when(g < n_groups)
        def _():
            each_block(jnp.int32(g), lambda copy: copy.start())

    ahead = (
        pltpu.make_async_copy(kc.at[:, me, pl.ds(0, SHORT), :], ks_out, next_sem.at[0]),
        pltpu.make_async_copy(vc.at[:, me, pl.ds(0, SHORT), :], vs_out, next_sem.at[1]),
        pltpu.make_async_copy(wo, wo_out, next_sem.at[2]),
    )
    def spread(b, carry):
        lv_out[pl.ds(b, 1), :] = jnp.full((1, hd), lens[b], jnp.int32)
        return carry

    lax.fori_loop(0, batch, spread, 0, unroll=8)

    for i in range(K_CHUNKS):
        for copy in loads(i):
            copy.wait()
        xs = xbuf[i]
        q_part = jnp.dot(xs, wqbuf[i], preferred_element_type=F32)
        k_part = jnp.dot(xs, wkbuf[i], preferred_element_type=F32)
        v_part = jnp.dot(xs, wvbuf[i], preferred_element_type=F32)
        for h in range(heads):
            piece = q_part[:, h * hd:(h + 1) * hd]
            q_out[h] = piece if i == 0 else q_out[h] + piece
        k1_out[...] = k_part if i == 0 else k1_out[...] + k_part
        v1_out[...] = v_part if i == 0 else v1_out[...] + v_part
    for copy in ahead:
        copy.start()

    q_out[...] = q_out[...].astype(BF16).astype(F32)
    k1_out[...] = k1_out[...].astype(BF16).astype(F32)
    v1_out[...] = v1_out[...].astype(BF16).astype(F32)

    def attend(g, carry):
        slot = lax.rem(g, RING)
        each_block(g, lambda copy: copy.wait())
        for j in range(PER_GROUP):
            b = sequence(g, j)
            length = lens[b]
            row = pl.ds(b, 1)
            q = jnp.concatenate([q_out[h, row, :] for h in range(heads)] * 2, axis=0)
            k1, v1 = k1_out[row, :], v1_out[row, :]
            s = lax.dot_general(q.astype(BF16), kbuf[slot, j], NT, preferred_element_type=F32) * scale
            s_new = jnp.sum(q * k1, axis=-1, keepdims=True) * scale
            s = jnp.where(lax.broadcasted_iota(jnp.int32, s.shape, 1) < length, s, -jnp.inf)
            m = jnp.maximum(jnp.max(s, axis=-1, keepdims=True), s_new)
            e = jnp.exp(s - m)
            e_new = jnp.exp(s_new - m)
            total = jnp.sum(e, axis=-1, keepdims=True) + e_new
            ebuf[j] = e.astype(BF16)
            nbuf[j] = e_new.astype(BF16).astype(F32) * v1
            tbuf[j] = jnp.broadcast_to(total, (8, hd))

        @pl.when(g < n_groups)
        def _():
            for j in range(PER_GROUP):
                row = pl.ds(sequence(g, j), 1)
                o = jnp.dot(ebuf[j], vbuf[slot, j], preferred_element_type=F32)
                o = (o + nbuf[j]) / tbuf[j]
                for h in range(heads):
                    ol_out[h, row, :] = o[h:h + 1, :]

        @pl.when(g + RING < n_groups)
        def _():
            each_block(g + RING, lambda copy: copy.start())

        return carry

    lax.fori_loop(0, n_groups, attend, 0)
    for copy in ahead:
        copy.wait()


def attend_short_and_reduce(
    q_ref, k1_ref, v1_ref, ol_ref, lv_ref, kbuf, vbuf, wobuf, x, wk, wv,
    y_out, kn_out, vn_out,
    xbuf, wkv, ebuf, nbuf, tbuf, obuf, part, got_core, got_one, got_two, kvbuf,
    load_sem, send_sem, recv_sem,
):
    me = lax.axis_index("model")
    core = me % 2
    px = (me // 2) % 2
    py = me // 4
    flip_x = me + 2 - 4 * px
    flip_y = me + 4 - 8 * py
    other_core = 1 - core
    partner = me + 1 - 2 * core
    across = flip_x + 4 - 8 * py
    near_one = other_core * flip_x + core * flip_y
    near_two = other_core * flip_y + core * flip_x
    a = other_core * px + core * py
    b = other_core * py + core * px
    base = 4 * core
    mine = base + 2 * a + b
    heads, batch, hd = q_ref.shape
    width = part.shape[2]
    kv_width = wkv.shape[1] // 2
    kv_heads = kv_width // hd
    slice_heads = 2 * kv_heads // KV_STEPS
    scale = hd ** -0.5

    loads = (
        pltpu.make_async_copy(x, xbuf, load_sem.at[0]),
        pltpu.make_async_copy(wk, wkv.at[:, pl.ds(0, kv_width)], load_sem.at[1]),
        pltpu.make_async_copy(wv, wkv.at[:, pl.ds(kv_width, kv_width)], load_sem.at[2]),
    )
    for copy in loads:
        copy.start()

    barrier = pltpu.get_barrier_semaphore()
    for other in (partner, near_one, near_two, across):
        pl.semaphore_signal(barrier, inc=1, device_id={"model": other}, device_id_type=pl.DeviceIdType.MESH)

    def rows_of(r):
        first, count = CHUNKS[r]
        return pl.ds(first, count)

    def cols_of(f, count):
        return pl.ds(pl.multiple_of(f * width, width), count * width)

    def send(stage, r):
        rows = rows_of(r)
        if stage == 0:
            src, dst, other = part.at[pl.ds(4 * other_core, 4), rows], got_core.at[:, rows], partner
        elif stage == 1 and r in DIRECT_SUM:
            src, dst, other = part.at[base + 2 * (1 - a) + b, rows], got_one.at[0, rows], near_one
        elif stage == 1:
            src, dst, other = part.at[pl.ds(base + 2 * (1 - a), 2), rows], got_one.at[:, rows], near_one
        elif stage == 2:
            src, dst, other = part.at[base + 2 * a + 1 - b, rows], got_two.at[rows], near_two
        elif stage == 6:
            src, dst, other = part.at[base + 2 * (1 - a) + 1 - b, rows], got_one.at[1, rows], across
        elif stage == 3:
            src = dst = y_out.at[rows, cols_of(mine, 1)]
            other = near_two
        elif stage == 7 or (stage == 4 and r in DIRECT_SHARE):
            src = dst = y_out.at[rows, cols_of(mine, 1)]
            other = across if stage == 7 else near_one
        elif stage == 4:
            src = dst = y_out.at[rows, cols_of(base + 2 * a, 2)]
            other = near_one
        else:
            src = dst = y_out.at[rows, cols_of(base, 4)]
            other = partner
        return pltpu.make_async_remote_copy(
            src_ref=src, dst_ref=dst, send_sem=send_sem.at[stage, r], recv_sem=recv_sem.at[stage, r],
            device_id={"model": other}, device_id_type=pl.DeviceIdType.MESH,
        )

    def advance(stage, r):
        rows = rows_of(r)
        send(stage, r).wait()
        following = (stage + 1,) if stage < 5 else ()
        if stage == 0:
            part[pl.ds(base, 4), rows] += got_core[:, rows]
            if r in DIRECT_SUM:
                following = (6, 1, 2)
        elif stage == 1:
            if r in DIRECT_SUM:
                following = ()
            else:
                part[pl.ds(base + 2 * a, 2), rows] += got_one[:, rows]
        elif stage == 2:
            total = part[mine, rows] + got_two[rows]
            if r in DIRECT_SUM:
                send(6, r).wait()
                total = total + (got_one[0, rows] + got_one[1, rows])
            total = total + xbuf[rows, cols_of(mine, 1)].astype(F32)
            y_out[rows, cols_of(mine, 1)] = total.astype(BF16)
            if r in DIRECT_SHARE:
                following = (7, 3, 4)
        elif stage == 3 and r in DIRECT_SHARE:
            following = ()
        elif stage == 4 and r in DIRECT_SHARE:
            send(7, r).wait()
        for later in following:
            send(later, r).start()

    def weigh(group):
        rows = pl.ds(pl.multiple_of(group * 8, 8), 8)
        q = jnp.concatenate([q_ref[h, rows, :] for h in range(heads)], axis=0)
        k1 = jnp.concatenate([k1_ref[rows, :]] * heads, axis=0)
        v1 = jnp.concatenate([v1_ref[rows, :]] * heads, axis=0)
        lens = jnp.concatenate([lv_ref[rows, :]] * heads, axis=0)
        k = kbuf[rows].reshape(8 * SHORT, hd)
        s = lax.dot_general(q.astype(BF16), k, NT, preferred_element_type=F32) * scale
        s_new = jnp.sum(q * k1, axis=-1, keepdims=True) * scale
        lane = lax.broadcasted_iota(jnp.int32, s.shape, 1)
        line = lax.broadcasted_iota(jnp.int32, s.shape, 0)
        slot = lane - (line % 8) * SHORT
        wide = jnp.concatenate([lens] * (s.shape[1] // hd), axis=1)
        s = jnp.where((slot >= 0) & (slot < jnp.minimum(wide, SHORT)), s, -jnp.inf)
        m = jnp.maximum(jnp.max(s, axis=-1, keepdims=True), s_new)
        e = jnp.exp(s - m)
        e_new = jnp.exp(s_new - m)
        total = jnp.sum(e, axis=-1, keepdims=True) + e_new
        ebuf[group] = e.astype(BF16)
        nbuf[group] = e_new.astype(BF16).astype(F32) * v1
        tbuf[group] = jnp.broadcast_to(total, (8 * heads, hd))

    def gather(group):
        rows = pl.ds(pl.multiple_of(group * 8, 8), 8)
        v = vbuf[rows].reshape(8 * SHORT, hd)
        o = jnp.dot(ebuf[group], v, preferred_element_type=F32)
        o = (o + nbuf[group]) / tbuf[group]
        long = lv_ref[rows, :] > SHORT
        for h in range(heads):
            obuf[rows, pl.ds(h * hd, hd)] = jnp.where(long, ol_ref[h, rows, :], o[h * 8:(h + 1) * 8])

    def attend(first, count):
        for act in (weigh, gather):
            def body(i, carry):
                for g in range(UNROLL):
                    act(first // 8 + i * UNROLL + g)
                return carry

            lax.fori_loop(0, count // 8 // UNROLL, body, 0)

    def project_out(first, count):
        rows = pl.ds(first, count)
        o_rows = obuf[rows, :].astype(BF16)
        for f in range(8):
            part[f, rows] = jnp.dot(o_rows, wobuf[:, f * width:(f + 1) * width], preferred_element_type=F32)

    def new_rows(t):
        if t == 0:
            loads[0].wait()
            loads[1].wait()
            loads[2].wait()
        cols = pl.ds(t * slice_heads * hd, slice_heads * hd)
        fresh = jnp.dot(xbuf[...], wkv[:, cols], preferred_element_type=F32)
        for h in range(slice_heads):
            kvbuf[:, (t * slice_heads + h) % kv_heads, :] = fresh[:, h * hd:(h + 1) * hd]
        if t == KV_STEPS // 2 - 1:
            kn_out[...] = kvbuf[...].astype(BF16)
        if t == KV_STEPS - 1:
            vn_out[...] = kvbuf[...].astype(BF16)

    for op, i in ORDER:
        if op == ATTEND:
            attend(*PARTS[i])
        elif op == PROJECT:
            project_out(*PARTS[i])
            if i == 0:
                pl.semaphore_wait(barrier, 4)
            for r, (first, _) in enumerate(CHUNKS):
                if PARTS[i][0] <= first < PARTS[i][0] + PARTS[i][1]:
                    send(0, r).start()
        elif op == NEW:
            new_rows(i)
        else:
            advance(op, i)


def copy_out(y, kn, vn, y_out, kn_out, vn_out, sem):
    copies = [
        pltpu.make_async_copy(src, dst, sem.at[i])
        for i, (src, dst) in enumerate(((y, y_out), (kn, kn_out), (vn, vn_out)))
    ]
    for copy in copies:
        copy.start()
    for copy in copies:
        copy.wait()


def solution(mesh):
    def local_step(x, w_query, w_key, w_value, w_out, k_cache, v_cache, lengths):
        batch, width = x.shape
        kv_heads, context, hd = k_cache.shape[1:]
        heads = w_query.shape[1] // hd
        kv_width = kv_heads * hd
        depth = width // K_CHUNKS
        piece = width // 8
        vmem = pl.BlockSpec(memory_space=pltpu.VMEM)
        hbm = pl.BlockSpec(memory_space=pltpu.HBM)
        sds = jax.ShapeDtypeStruct
        x, w_query, w_key, w_value, w_out, k_cache, v_cache, lengths = (
            pltpu.with_memory_space_constraint(array, pltpu.HBM)
            for array in (x, w_query, w_key, w_value, w_out, k_cache, v_cache, lengths)
        )

        ahead = pl.pallas_call(
            project_and_attend_long,
            out_shape=(
                sds((heads, batch, hd), F32), sds((batch, hd), F32), sds((batch, hd), F32),
                sds((heads, batch, hd), F32), sds((batch, hd), jnp.int32),
                sds((batch, SHORT, hd), BF16), sds((batch, SHORT, hd), BF16), sds((heads * hd, width), BF16),
            ),
            in_specs=[hbm] * 8,
            out_specs=[vmem] * 8,
            scratch_shapes=[
                pltpu.VMEM((K_CHUNKS, batch, depth), BF16),
                pltpu.VMEM((K_CHUNKS, depth, heads * hd), BF16),
                pltpu.VMEM((K_CHUNKS, depth, hd), BF16),
                pltpu.VMEM((K_CHUNKS, depth, hd), BF16),
                pltpu.VMEM((RING, PER_GROUP, context, hd), BF16),
                pltpu.VMEM((RING, PER_GROUP, context, hd), BF16),
                pltpu.VMEM((PER_GROUP, 8, context), BF16),
                pltpu.VMEM((PER_GROUP, 8, hd), F32),
                pltpu.VMEM((PER_GROUP, 8, hd), F32),
                pltpu.SMEM((batch,), jnp.int32),
                pltpu.SMEM((batch,), jnp.int32),
                pltpu.SemaphoreType.DMA((K_CHUNKS, 5)),
                pltpu.SemaphoreType.DMA((RING, PER_GROUP, context // BLOCK)),
                pltpu.SemaphoreType.DMA((RING, PER_GROUP, context // BLOCK)),
                pltpu.SemaphoreType.DMA((3,)),
            ],
            compiler_params=pltpu.CompilerParams(vmem_limit_bytes=28 * 2**20),
            name="project_and_attend_long",
        )(lengths, x, w_query, w_key, w_value, w_out, k_cache, v_cache)

        new_shape = (batch, kv_heads, hd)
        result = (sds((batch, width), BF16), sds(new_shape, BF16), sds(new_shape, BF16))
        held = pl.pallas_call(
            attend_short_and_reduce,
            out_shape=result,
            in_specs=[vmem] * 8 + [hbm] * 3,
            out_specs=[vmem] * 3,
            scratch_shapes=[
                pltpu.VMEM((batch, width), BF16),
                pltpu.VMEM((width, 2 * kv_width), BF16),
                pltpu.VMEM((batch // 8, 8 * heads, 8 * SHORT), BF16),
                pltpu.VMEM((batch // 8, 8 * heads, hd), F32),
                pltpu.VMEM((batch // 8, 8 * heads, hd), F32),
                pltpu.VMEM((batch, heads * hd), F32),
                pltpu.VMEM((8, batch, piece), F32),
                pltpu.VMEM((4, batch, piece), F32),
                pltpu.VMEM((2, batch, piece), F32),
                pltpu.VMEM((batch, piece), F32),
                pltpu.VMEM(new_shape, F32),
                pltpu.SemaphoreType.DMA((3,)),
                pltpu.SemaphoreType.DMA((8, len(CHUNKS))),
                pltpu.SemaphoreType.DMA((8, len(CHUNKS))),
            ],
            compiler_params=pltpu.CompilerParams(
                vmem_limit_bytes=40 * 2**20, collective_id=0, has_side_effects=True
            ),
            name="attend_short_and_reduce",
        )(*ahead, x, w_key, w_value)
        return pl.pallas_call(
            copy_out,
            out_shape=result,
            in_specs=[vmem] * 3,
            out_specs=[pl.BlockSpec(memory_space=pltpu.HBM)] * 3,
            scratch_shapes=[pltpu.SemaphoreType.DMA((3,))],
            compiler_params=pltpu.CompilerParams(vmem_limit_bytes=2**20),
            name="copy_out",
        )(*held)

    rows_spec = P("replica")
    return jax.shard_map(
        local_step,
        mesh=mesh,
        in_specs=(P("replica", None), P(None, "model"), P(), P(), P("model", None), rows_spec, rows_spec, rows_spec),
        out_specs=(rows_spec, rows_spec, rows_spec),
        check_vma=False,
    )
```
